512 devices in a mesh: grp: 16 (over y, x_lo), row: 8 (over z), col: 4 (over x_hi, core).
Axes of the slice: x: 4 (x_hi: 2, x_lo: 2; x = x_hi * 2 + x_lo), y: 8, z: 8, core: 2. Of those that a mesh axis runs over, the one named last changes fastest.
Arguments:
- normals: float32 [16, 4096, 4096], P('grp', 'row', 'col'), as said below
- transforms: float32 [16, 32, 128, 128], P('grp', 'row'), as said below
- block_map: int32 [16, 32], P('grp'), may hold values from 0 to 31, as said below
Outputs:
- eliminated: float32 [4096, 4096], P('row', 'col')
The draws below stay inside these ranges and needn't reach their ends.
Inputs may be any that keep to these rules, and one draw needn't show every extreme that they name: `block_map`: for each group, a permutation of the blocks that maps every aligned range of 4 blocks onto itself. `normals`: each group's matrix is symmetric positive definite. `transforms`: each block is nonsingular.
All inputs are finite; a program needn't handle non-finite values.
Results may differ from the reference program's by a relative error of at most 0.0001.
Values sent between devices are 32-bit elements; how exact they have to be, the bound alone decides.
A program may use at most 64 MiB of HBM per device.

```python
import jax
import jax.numpy as jnp
from jax import lax

P_SIZE = 4096
BLK = 128
NPAN = 5
GROUPS = 16
NB = 32
SPAN = 4


loading_count = 64


def draw_normals(key, part):
    key_noise = jax.random.fold_in(key, 0)
    key_scale = jax.random.fold_in(key, 1)
    key_loading = jax.random.fold_in(key, 3)
    noise_field = jax.random.normal(key_noise, (GROUPS, P_SIZE, P_SIZE), jnp.float32)
    scales = jnp.exp(jax.random.uniform(key_scale, (GROUPS, P_SIZE), jnp.float32, jnp.log(0.3), jnp.log(3.0)))
    loadings = jax.random.normal(key_loading, (GROUPS, P_SIZE, loading_count), jnp.float32)
    loadings = loadings * jnp.sqrt(3.0 / loading_count)
    shared = jnp.einsum('gpr,gqr->gpq', loadings, loadings, precision=lax.Precision.HIGHEST)
    symmetric = (noise_field + jnp.swapaxes(noise_field, 1, 2)) / jnp.sqrt(2.0 * P_SIZE)
    base_core = symmetric + shared + 3.0 * jnp.eye(P_SIZE, dtype=jnp.float32)[None]
    return scales[:, :, None] * base_core * scales[:, None, :] / GROUPS


def draw_transforms(key, part):
    noise_blocks = jax.random.normal(key, (GROUPS, NB, BLK, BLK), jnp.float32)
    return jnp.eye(BLK, dtype=jnp.float32)[None, None] + 0.5 / jnp.sqrt(1.0 * BLK) * noise_blocks


def draw_block_map(key, part):
    sort_scores = jax.random.randint(key, (GROUPS, NB // SPAN, SPAN), 0, 2 ** 20)
    sort_scores = sort_scores * SPAN + jnp.arange(SPAN, dtype=jnp.int32)[None, None, :]
    block_order = jnp.argsort(sort_scores, axis=2, stable=True).astype(jnp.int32)
    range_starts = (jnp.arange(NB // SPAN, dtype=jnp.int32) * SPAN)[None, :, None]
    return (block_order + range_starts).reshape(GROUPS, NB)


def setup_inputs(seed: int = 0) -> dict:
    arg_keys = jax.random.split(jax.random.key(seed), 4)
    return {
        "normals": draw_normals(jax.random.fold_in(arg_keys[3], 71), 0),
        "transforms": draw_transforms(jax.random.fold_in(arg_keys[3], 71), 0),
        "block_map": draw_block_map(jax.random.fold_in(arg_keys[3], 71), 0),
    }


def transform_group(normal, blocks, mapping):
    nblocks = P_SIZE // BLK
    grid = normal.reshape(nblocks, BLK, nblocks, BLK)
    half_done = jnp.einsum('aij,aibk->ajbk', blocks, grid, precision=lax.Precision.HIGHEST)
    rotated = jnp.einsum('ajbk,bkl->ajbl', half_done, blocks, precision=lax.Precision.HIGHEST)
    rotated = jnp.take(rotated, mapping.astype(jnp.int32), axis=0)
    rotated = jnp.take(rotated, mapping.astype(jnp.int32), axis=2)
    return rotated.reshape(P_SIZE, P_SIZE)

def reference(normals, transforms, block_map):

    def add_group(group, combined):
        return combined + transform_group(normals[group], transforms[group], block_map[group])
    matrix = lax.fori_loop(0, GROUPS, add_group, jnp.zeros((P_SIZE, P_SIZE), jnp.float32))
    for panel in range(NPAN):
        offset = panel * BLK
        column = matrix[:, offset:offset + BLK]
        factor_block = jnp.linalg.cholesky(column[offset:offset + BLK])
        factor = lax.linalg.triangular_solve(factor_block, column, left_side=False, lower=True, transpose_a=True)
        below = jnp.arange(P_SIZE)[:, None] >= offset
        factor = jnp.where(below, factor, jnp.zeros_like(factor))
        matrix = matrix - jnp.dot(factor.astype(jnp.float32), factor.T.astype(jnp.float32), precision=lax.Precision.HIGHEST, preferred_element_type=jnp.float32)
        matrix = matrix.at[:, offset:offset + BLK].set(factor)
    return matrix
```

```python
import functools

import jax
import jax.numpy as jnp
from jax import lax
from jax.experimental import pallas as pl
from jax.experimental.pallas import tpu as pltpu
from jax.sharding import PartitionSpec as P

BLK = 128
NPAN = 5
STEP = 8
MESH = pl.DeviceIdType.MESH
HIGHEST = lax.Precision.HIGHEST
VMEM = pl.BlockSpec(memory_space=pltpu.VMEM)
PAIRS = [(i, j) for i in range(NPAN) for j in range(i, NPAN)]
NPAIR = len(PAIRS)


def f32(*shape):
    return jax.ShapeDtypeStruct(shape, jnp.float32)


def place():
    grp = lax.axis_index("grp")
    col = lax.axis_index("col")
    return dict(
        g=grp, y=grp // 2, xl=grp % 2, z=lax.axis_index("row"), c=col, xh=col // 2, core=col % 2
    )


def remote(src, dst, send, recv, **where):
    return pltpu.make_async_remote_copy(
        src_ref=src, dst_ref=dst, send_sem=send, recv_sem=recv, device_id=where, device_id_type=MESH
    )


def arrived(dst, send, recv):
    remote(dst, dst, send, recv, grp=lax.axis_index("grp")).wait_recv()


def meet(partners):
    barrier = pltpu.get_barrier_semaphore()
    for where in partners:
        pl.semaphore_signal(barrier, inc=1, device_id=where, device_id_type=MESH)
    pl.semaphore_wait(barrier, len(partners))


def params(ident):
    return pltpu.CompilerParams(collective_id=ident, has_side_effects=True, vmem_limit_bytes=40 << 20)


def spread_transforms_kernel(own, out, send_r, send_l, recv, sem):
    me = place()
    z, c, core = me["z"], me["c"], me["core"]
    right, left = (z + 1) % 8, (z + 7) % 8
    reach = 4 - core
    meet([{"row": right}, {"row": left}])
    for part in range(4):
        for slot in range(2):
            index = slot * 4 + part
            away = (z - (2 * c + slot) + 8) % 8
            here = out.at[index]

            def copy(src, sends, to):
                return remote(src, here, sends.at[index], recv.at[index], row=to)

            @pl.when(away == 0)
            def _():
                copy(own.at[part], send_r, right).start()
                copy(own.at[part], send_l, left).start()
                out[index] = own[part]

            @pl.when(away != 0)
            def _():
                arrived(here, send_r.at[index], recv.at[index])

            @pl.when((away > 0) & (away < reach))
            def _():
                copy(here, send_r, right).start()

            @pl.when(away > reach + 1)
            def _():
                copy(here, send_l, left).start()

    for part in range(4):
        for slot in range(2):
            index = slot * 4 + part
            away = (z - (2 * c + slot) + 8) % 8
            here = out.at[index]

            @pl.when(away < reach)
            def _():
                remote(here, here, send_r.at[index], recv.at[index], row=right).wait_send()

            @pl.when((away > reach + 1) | (away == 0))
            def _():
                remote(here, here, send_l.at[index], recv.at[index], row=left).wait_send()


def spread_transforms(own):
    return pl.pallas_call(
        spread_transforms_kernel,
        out_shape=f32(8, BLK, BLK),
        in_specs=[VMEM],
        out_specs=VMEM,
        scratch_shapes=[pltpu.SemaphoreType.DMA((8,))] * 3 + [pltpu.SemaphoreType.DMA],
        compiler_params=params(1),
    )(own)


def transform_kernel(rows, cols, normal, row_t, col_t, out, half):
    i = pl.program_id(0)
    left = row_t[rows[i]].T
    moved = jnp.dot(left, normal[...], precision=HIGHEST, preferred_element_type=jnp.float32)
    for b in range(8):
        half[b] = moved[:, b * BLK : (b + 1) * BLK]
    for j in range(8):
        b = cols[j]
        out[0, j] = jnp.dot(half[b], col_t[b], precision=HIGHEST, preferred_element_type=jnp.float32)


def transform(normal, row_t, col_t, rows, cols):
    return pl.pallas_call(
        transform_kernel,
        out_shape=f32(4, 8, BLK, BLK),
        grid_spec=pltpu.PrefetchScalarGridSpec(
            num_scalar_prefetch=2,
            grid=(4,),
            in_specs=[
                pl.BlockSpec((BLK, 1024), lambda i, r, c: (r[i], 0)),
                pl.BlockSpec((4, BLK, BLK), lambda i, r, c: (0, 0, 0)),
                pl.BlockSpec((8, BLK, BLK), lambda i, r, c: (0, 0, 0)),
            ],
            out_specs=pl.BlockSpec((1, 8, BLK, BLK), lambda i, r, c: (i, 0, 0, 0)),
            scratch_shapes=[pltpu.VMEM((8, BLK, BLK), jnp.float32)],
        ),
        compiler_params=pltpu.CompilerParams(vmem_limit_bytes=40 << 20),
    )(rows, cols, normal, row_t, col_t)


def leading_kernel(moved, out, parts, extra, total, s1, r1, se, re, s2, r2, s3, r3, s4, r4):
    me = place()
    g, z, c, xh, core = me["g"], me["z"], me["c"], me["xh"], me["core"]
    first = (z == 0) & (c == 0)
    partners = [{"grp": (g + d) % 16} for d in range(1, 16)]
    partners += [{"row": (z + d) % 8} for d in range(1, 8)]
    partners += [{"col": c ^ 1}, {"col": c ^ 2}]
    meet(partners)
    last = PAIRS.index((4, 4))

    @pl.when((z == 1) & (c == 0))
    def _():
        remote(moved.at[0, 4], extra, se, re, row=0).start()
        remote(moved.at[0, 4], extra, se, re, row=0).wait_send()

    @pl.when(first)
    def _():
        for t, (i, j) in enumerate(PAIRS):
            if t == last:
                arrived(extra, se, re)
                src = extra
            else:
                src = moved.at[i, j]

            @pl.when(g != t)
            def _():
                remote(src, parts.at[g], s1.at[t], r1.at[g], grp=t).start()

            @pl.when(g == t)
            def _():
                total[...] = src[...]

        @pl.when(g < NPAIR)
        def _():
            for d in range(1, 16):
                arrived(parts.at[(g + d) % 16], s1.at[0], r1.at[(g + d) % 16])
            acc = total[...]
            for d in range(1, 16):
                acc = acc + parts[(g + d) % 16]
            total[...] = acc
            out[g] = acc

        for t, (i, j) in enumerate(PAIRS):
            @pl.when(g != t)
            def _():
                remote(extra, parts.at[g], s1.at[t], r1.at[g], grp=t).wait_send()

    @pl.when(g < NPAIR)
    def _():
        @pl.when((z == 0) & (core == 0))
        def _():
            @pl.when(c == 0)
            def _():
                remote(total, out.at[g], s2.at[0], r2, col=2).start()
                for d in range(1, 8):
                    remote(total, out.at[g], s2.at[d], r2, row=(z + d) % 8).start()
                for d in range(8):
                    remote(total, out.at[g], s2.at[d], r2, row=(z + 1) % 8).wait_send()

            @pl.when(c == 2)
            def _():
                arrived(out.at[g], s2.at[0], r2)
                for d in range(1, 8):
                    remote(out.at[g], out.at[g], s2.at[d], r2, row=(z + d) % 8).start()
                for d in range(1, 8):
                    remote(out.at[g], out.at[g], s2.at[d], r2, row=(z + 1) % 8).wait_send()

        @pl.when((z != 0) & (core == 0))
        def _():
            arrived(out.at[g], s2.at[0], r2)

    @pl.when(core == 0)
    def _():
        @pl.when(g < NPAIR)
        def _():
            for d in (8, 7, 9, 6, 10, 5, 11, 4, 12, 3, 13, 2, 14, 1, 15):
                remote(out.at[g], out.at[g], s3.at[d], r3.at[g], grp=(g + d) % 16).start()
            remote(out.at[g], out.at[g], s4.at[0], r4.at[g], col=c ^ 1).start()
        for d in range(1, 16):
            t = (g + d) % 16

            @pl.when(t < NPAIR)
            def _():
                arrived(out.at[t], s3.at[0], r3.at[t])
                remote(out.at[t], out.at[t], s4.at[d], r4.at[t], col=c ^ 1).start()

        @pl.when(g < NPAIR)
        def _():
            for d in range(1, 16):
                remote(out.at[g], out.at[g], s3.at[d], r3.at[g], grp=(g + d) % 16).wait_send()
        for d in range(16):
            t = (g + d) % 16

            @pl.when(t < NPAIR)
            def _():
                remote(out.at[t], out.at[t], s4.at[d], r4.at[t], col=c ^ 1).wait_send()

    @pl.when(core == 1)
    def _():
        for t in range(NPAIR):
            arrived(out.at[t], s4.at[0], r4.at[t])


def leading(moved):
    dma = pltpu.SemaphoreType.DMA
    return pl.pallas_call(
        leading_kernel,
        out_shape=f32(NPAIR, BLK, BLK),
        in_specs=[VMEM],
        out_specs=VMEM,
        scratch_shapes=[
            pltpu.VMEM((16, BLK, BLK), jnp.float32),
            pltpu.VMEM((BLK, BLK), jnp.float32),
            pltpu.VMEM((BLK, BLK), jnp.float32),
            dma((16,)), dma((16,)), dma, dma, dma((8,)), dma, dma((16,)), dma((16,)), dma((16,)), dma((16,)),
        ],
        compiler_params=params(2),
    )(moved)


def add_up_kernel(moved, out, half, mine, parts, sx, rx, sy, ry):
    me = place()
    g, y, xl = me["g"], me["y"], me["xl"]
    order = (4, 1, 7, 2, 6, 3, 5, 0)
    meet([{"grp": g ^ 1}] + [{"grp": (g + 2 * d) % 16} for d in range(1, 8)])

    def across(d):
        b = (y + d) % 8
        return remote(moved.at[pl.ds(2 * (1 - xl), 2), b], half.at[b], sx.at[d], rx.at[d], grp=g ^ 1)

    def along(d):
        b = (y + d) % 8
        return remote(mine.at[b], parts.at[d], sy.at[d], ry.at[d], grp=(g + 2 * d) % 16)

    for d in order:
        across(d).start()
    for d in order:
        b = (y + d) % 8
        across(d).wait_recv()
        mine[b] = moved[pl.ds(2 * xl, 2), b] + half[b]
        if d:
            along(d).start()
    acc = mine[y]
    for d in order[:-1]:
        along(d).wait_recv()
        acc = acc + parts[d]
    out[...] = acc
    for d in order:
        across(d).wait_send()
        if d:
            along(d).wait_send()


def add_up(moved):
    dma = pltpu.SemaphoreType.DMA
    return pl.pallas_call(
        add_up_kernel,
        out_shape=f32(2, BLK, BLK),
        in_specs=[VMEM],
        out_specs=VMEM,
        scratch_shapes=[pltpu.VMEM((8, 2, BLK, BLK), jnp.float32)] * 3 + [dma((8,))] * 4,
        compiler_params=params(3),
    )(moved)


def panels_kernel(own, by_row, by_col, sx, rr, sy, sc, rc_d2d, sz, rz, sl, rl):
    me = place()
    g, y, xl, z, c, core = me["g"], me["y"], me["xl"], me["z"], me["c"], me["core"]
    partners = [{"grp": (g + 2 * d) % 16} for d in range(1, 8)] + [{"grp": g ^ 1}]
    partners += [{"row": (z + d) % 8} for d in range(1, 8)] + [{"col": c ^ 1}, {"col": c ^ 2}]
    meet(partners)

    for src_z, src_xl, start, count in ((0, 0, 0, 2), (0, 1, 2, 2), (1, 0, 4, 1)):
        n = src_z * 2 + src_xl
        there = by_col.at[pl.ds(start, count)]
        src = own.at[pl.ds(0, count)]

        @pl.when((z == src_z) & (xl == src_xl))
        def _():
            for d in range(1, 8):
                remote(src, there, sz.at[n, d], rz.at[n], row=(z + d) % 8).start()
            remote(src, there, sl.at[n], rl.at[n], grp=g ^ 1).start()
            by_col[start : start + count] = own[0:count]

    @pl.when((c == 0) & (y < NPAN))
    def _():
        remote(own, by_row.at[y], sx, rr.at[y], col=2).start()
        for d in (4, 3, 5, 2, 6, 1, 7):
            remote(own, by_row.at[y], sy.at[d], rr.at[y], grp=(g + 2 * d) % 16).start()
        by_row[y] = own[...]

    @pl.when((c == 2) & (y < NPAN))
    def _():
        arrived(by_row.at[y], sx, rr.at[y])
        for d in (4, 3, 5, 2, 6, 1, 7):
            remote(by_row.at[y], by_row.at[y], sy.at[d], rr.at[y], grp=(g + 2 * d) % 16).start()

    @pl.when(core == 0)
    def _():
        for k in range(NPAN):
            @pl.when((y == k) & (c == 0))
            def _():
                remote(own, by_row.at[k], sc.at[k], rc_d2d.at[k], col=c ^ 1).start()

            @pl.when((y == k) & (c == 2))
            def _():
                remote(by_row.at[k], by_row.at[k], sc.at[k], rc_d2d.at[k], col=c ^ 1).start()

            @pl.when(y != k)
            def _():
                arrived(by_row.at[k], sx, rr.at[k])
                remote(by_row.at[k], by_row.at[k], sc.at[k], rc_d2d.at[k], col=c ^ 1).start()

    for src_z, src_xl, start, count in ((0, 0, 0, 2), (0, 1, 2, 2), (1, 0, 4, 1)):
        n = src_z * 2 + src_xl
        there = by_col.at[pl.ds(start, count)]

        @pl.when((z != src_z) & (xl == src_xl))
        def _():
            arrived(there, sz.at[n, 0], rz.at[n])
            remote(there, there, sl.at[n], rl.at[n], grp=g ^ 1).start()

        @pl.when(xl != src_xl)
        def _():
            arrived(there, sl.at[n], rl.at[n])

    @pl.when(core == 1)
    def _():
        for k in range(NPAN):
            arrived(by_row.at[k], sc.at[k], rc_d2d.at[k])

    for src_z, src_xl, start, count in ((0, 0, 0, 2), (0, 1, 2, 2), (1, 0, 4, 1)):
        n = src_z * 2 + src_xl
        there = by_col.at[pl.ds(start, count)]

        @pl.when(xl == src_xl)
        def _():
            @pl.when(z == src_z)
            def _():
                for d in range(1, 8):
                    remote(there, there, sz.at[n, d], rz.at[n], row=(z + d) % 8).wait_send()
            remote(there, there, sl.at[n], rl.at[n], grp=g ^ 1).wait_send()

    @pl.when((core == 0) & (y < NPAN))
    def _():
        @pl.when(c == 0)
        def _():
            remote(own, by_row.at[y], sx, rr.at[y], col=2).wait_send()
        for d in range(1, 8):
            remote(own, by_row.at[y], sy.at[d], rr.at[y], grp=(g + 2 * d) % 16).wait_send()

    @pl.when(core == 0)
    def _():
        for k in range(NPAN):
            remote(own, by_row.at[k], sc.at[k], rc_d2d.at[k], col=c ^ 1).wait_send()


def panels(own):
    dma = pltpu.SemaphoreType.DMA
    return pl.pallas_call(
        panels_kernel,
        out_shape=(f32(NPAN, 2, BLK, BLK), f32(NPAN, BLK, BLK)),
        in_specs=[VMEM],
        out_specs=(VMEM, VMEM),
        scratch_shapes=[
            dma, dma((NPAN,)), dma((8,)), dma((NPAN,)), dma((NPAN,)), dma((3, 8)), dma((3,)), dma((3,)), dma((3,)),
        ],
        compiler_params=params(4),
    )(own)


def factor_inverse(a):
    row_ids = lax.broadcasted_iota(jnp.int32, (BLK, BLK), 0)
    col_ids = lax.broadcasted_iota(jnp.int32, (BLK, BLK), 1)
    inv = jnp.where(row_ids == col_ids, 1.0, 0.0).astype(jnp.float32)
    done = []
    for start in range(0, BLK, STEP):
        rest = BLK - start
        cols = [jnp.broadcast_to(a[:, start + j : start + j + 1], (rest, BLK)) for j in range(STEP)]
        top_a, top_i = a[:STEP], inv[:STEP]
        rows_a, rows_i = [], []
        for j in range(STEP):
            scale = lax.rsqrt(cols[j][j : j + 1])
            cols[j] = cols[j] * scale
            row_a, row_i = top_a[j : j + 1] * scale, top_i[j : j + 1] * scale
            rows_a.append(row_a)
            rows_i.append(row_i)
            if j + 1 < STEP:
                low = cols[j][:STEP]
                top_a = top_a - low * row_a
                top_i = top_i - low * row_i
                for k in range(j + 1, STEP):
                    cols[k] = cols[k] - cols[j][k : k + 1] * cols[j]
        done.append(jnp.concatenate(rows_i, axis=0))
        if rest > STEP:
            a, inv = a[STEP:], inv[STEP:]
            for j in range(STEP):
                low = cols[j][STEP:]
                a = a - low * rows_a[j]
                inv = inv - low * rows_i[j]
    return jnp.concatenate(done, axis=0)


def mm(a, b):
    return jnp.dot(a, b, precision=HIGHEST, preferred_element_type=jnp.float32)


def mm_nt(a, b):
    return lax.dot_general(
        a, b, (((1,), (1,)), ((), ())), precision=HIGHEST, preferred_element_type=jnp.float32
    )


def eliminate_kernel(lead, by_row, by_col, own, out, square, upper, rows, cols):
    me = place()
    row_block = 4 * me["z"] + 2 * me["xl"]
    col_block = 8 * me["c"] + me["y"]
    for t, (i, j) in enumerate(PAIRS):
        square[i, j] = lead[t]
    rows[...] = by_row[...]
    cols[...] = by_col[...]
    out[...] = own[...]

    def panel(k, carry):
        inverse = factor_inverse(square[k, k])
        col_factor = mm(inverse, cols[k])
        row_factor = mm_nt(rows[k].reshape(2 * BLK, BLK), inverse)
        which = row_block + lax.broadcasted_iota(jnp.int32, (2 * BLK, BLK), 0) // BLK
        row_factor = jnp.where(which >= k, row_factor, 0.0)

        def solve(j, carry):
            upper[j] = mm(inverse, square[k, j])
            return carry

        lax.fori_loop(k + 1, NPAN, solve, 0)

        def update(i, carry):
            flipped = upper[i].T

            def inner(j, carry):
                square[i, j] -= mm(flipped, upper[j])
                return carry

            lax.fori_loop(i, NPAN, inner, 0)
            cols[i] -= mm(flipped, col_factor)
            rows[i] -= mm(row_factor, upper[i]).reshape(2, BLK, BLK)
            return carry

        lax.fori_loop(k + 1, NPAN, update, 0)

        @pl.when(col_block >= NPAN)
        def _():
            out[...] -= mm(row_factor, col_factor).reshape(2, BLK, BLK)

        @pl.when(col_block == k)
        def _():
            out[...] = row_factor.reshape(2, BLK, BLK)

        return carry

    lax.fori_loop(0, NPAN, panel, 0)


def eliminate(lead, by_row, by_col, own):
    return pl.pallas_call(
        eliminate_kernel,
        out_shape=f32(2, BLK, BLK),
        in_specs=[VMEM] * 4,
        out_specs=VMEM,
        scratch_shapes=[
            pltpu.VMEM((NPAN, NPAN, BLK, BLK), jnp.float32),
            pltpu.VMEM((NPAN, BLK, BLK), jnp.float32),
            pltpu.VMEM((NPAN, 2, BLK, BLK), jnp.float32),
            pltpu.VMEM((NPAN, BLK, BLK), jnp.float32),
        ],
        compiler_params=pltpu.CompilerParams(vmem_limit_bytes=40 << 20),
    )(lead, by_row, by_col, own)


def collect_kernel(own, out, sy, ry, sx, rx):
    me = place()
    g, y, xl = me["g"], me["y"], me["xl"]
    order = (1, 7, 2, 6, 3, 5, 4)
    meet([{"grp": g ^ 1}] + [{"grp": (g + 2 * d) % 16} for d in range(1, 8)])

    def spot(x, d):
        col = pl.multiple_of(((y - d + 8) % 8) * BLK, BLK)
        return out.at[pl.ds(pl.multiple_of(x * 2 * BLK, BLK), 2 * BLK), pl.ds(col, BLK)]

    def along(d):
        return remote(own, spot(xl, 0), sy.at[d], ry.at[d], grp=(g + 2 * d) % 16)

    def across(d, src):
        return remote(src, spot(xl, d), sx.at[d], rx.at[d], grp=g ^ 1)

    for d in (4, 3, 5, 2, 6, 1, 7):
        along(d).start()
    across(0, own).start()
    mine = pl.ds(pl.multiple_of(xl * 2 * BLK, BLK), 2 * BLK)
    out[mine, pl.ds(pl.multiple_of(y * BLK, BLK), BLK)] = own[...]
    for d in order:
        arrived(spot(xl, d), sy.at[d], ry.at[d])
        across(d, spot(xl, d)).start()
    for d in (0,) + order:
        arrived(spot(1 - xl, d), sx.at[d], rx.at[d])
    for d in (0,) + order:
        across(d, own).wait_send()
        if d:
            along(d).wait_send()


def collect(own):
    dma = pltpu.SemaphoreType.DMA
    return pl.pallas_call(
        collect_kernel,
        out_shape=f32(4 * BLK, 8 * BLK),
        in_specs=[VMEM],
        out_specs=VMEM,
        scratch_shapes=[dma((8,))] * 4,
        compiler_params=params(5),
    )(own)


def on_device(normals, transforms, block_map):
    row = lax.axis_index("row")
    col = lax.axis_index("col")
    mapping = block_map[0]
    row_map = lax.dynamic_slice_in_dim(mapping, row * 4, 4, 0) - row * 4
    col_map = lax.dynamic_slice_in_dim(mapping, col * 8, 8, 0) - col * 8
    col_transforms = spread_transforms(transforms[0])
    moved = transform(normals[0], transforms[0], col_transforms, row_map, col_map)
    lead = leading(moved)
    own = add_up(moved)
    by_row, by_col = panels(own)
    done = eliminate(lead, by_row, by_col, own)
    return collect(done.reshape(2 * BLK, BLK))


def solution(mesh):
    return jax.shard_map(
        on_device,
        mesh=mesh,
        in_specs=(P("grp", "row", "col"), P("grp", "row", None, None), P("grp", None)),
        out_specs=P("row", "col"),
        check_vma=False,
    )
```

```python
import functools

import jax
import jax.numpy as jnp
from jax import lax
from jax.experimental import pallas as pl
from jax.experimental.pallas import tpu as pltpu
from jax.sharding import PartitionSpec as P

BLK = 128
NPAN = 5
STEP = 8
MESH = pl.DeviceIdType.MESH
HIGHEST = lax.Precision.HIGHEST
VMEM = pl.BlockSpec(memory_space=pltpu.VMEM)
PAIRS = [(i, j) for i in range(NPAN) for j in range(i, NPAN)]
NPAIR = len(PAIRS)


def f32(*shape):
    return jax.ShapeDtypeStruct(shape, jnp.float32)


def place():
    grp = lax.axis_index("grp")
    col = lax.axis_index("col")
    return dict(
        g=grp, y=grp // 2, xl=grp % 2, z=lax.axis_index("row"), c=col, xh=col // 2, core=col % 2
    )


def remote(src, dst, send, recv, **where):
    return pltpu.make_async_remote_copy(
        src_ref=src, dst_ref=dst, send_sem=send, recv_sem=recv, device_id=where, device_id_type=MESH
    )


def arrived(dst, send, recv):
    remote(dst, dst, send, recv, grp=lax.axis_index("grp")).wait_recv()


def meet(partners):
    barrier = pltpu.get_barrier_semaphore()
    for where in partners:
        pl.semaphore_signal(barrier, inc=1, device_id=where, device_id_type=MESH)
    pl.semaphore_wait(barrier, len(partners))


def params(ident):
    return pltpu.CompilerParams(collective_id=ident, has_side_effects=True, vmem_limit_bytes=40 << 20)


FAR = (4, 3, 5, 2, 6, 1, 7)
GRP_FAR = (8, 7, 9, 6, 10, 5, 11, 4, 12, 3, 13, 2, 14, 1, 15)
COL_SOURCES = ((0, 0, 0, 2), (0, 1, 2, 2), (1, 0, 4, 1))


def dot(a, b):
    return jnp.dot(a, b, precision=HIGHEST, preferred_element_type=jnp.float32)


def gather_kernel(
    mapping, own_t, normal_hbm, lead, own, by_row, by_col,
    normal, col_t, left, moved, half, mine, parts, lparts, extra, total,
    sem, send_r, send_l, recv, sx, rx, sy, ry,
    s1, r1, se, re, s2, r2, s3, r3, s4, r4, spx, rr, spy, sc, rcd, sz, rz, sl, rl,
):
    me = place()
    g, y, xl, z, c, core = me["g"], me["y"], me["xl"], me["z"], me["c"], me["core"]
    fetch = pltpu.make_async_copy(normal_hbm, normal, sem)
    fetch.start()
    meet(
        [{"grp": (g + d) % 16} for d in range(1, 16)]
        + [{"row": (z + d) % 8} for d in range(1, 8)]
        + [{"col": c ^ 1}, {"col": c ^ 2}]
    )

    up, down = (z + 1) % 8, (z + 7) % 8
    reach = 4 - core

    def away_of(slot):
        return (z - (2 * c + slot) + 8) % 8

    def spread(index, src, sends, to):
        return remote(src, col_t.at[index], sends.at[index], recv.at[index], row=to)

    for slot in range(2):
        @pl.when(away_of(slot) == 0)
        def _():
            for part in range(4):
                index = slot * 4 + part
                spread(index, own_t.at[part], send_r, up).start()
                spread(index, own_t.at[part], send_l, down).start()
                col_t[index] = own_t[part]

    fetch.wait()
    for i in range(4):
        block = mapping[0, 4 * z + i] % 4
        turned = dot(own_t[block].T, normal[block])
        for b in range(8):
            left[b, i * BLK : (i + 1) * BLK, :] = turned[:, b * BLK : (b + 1) * BLK]

    rising = (away_of(1) <= reach).astype(jnp.int32)
    for part in range(4):
        for turn in range(2):
            slot = (rising + turn) % 2
            index = slot * 4 + part
            away = away_of(slot)

            @pl.when(away != 0)
            def _():
                arrived(col_t.at[index], send_r.at[index], recv.at[index])

            @pl.when((away > 0) & (away < reach))
            def _():
                spread(index, col_t.at[index], send_r, up).start()

            @pl.when(away > reach + 1)
            def _():
                spread(index, col_t.at[index], send_l, down).start()

    order = (4, 1, 7, 2, 6, 3, 5, 0)

    def across(d):
        b = (y + d) % 8
        return remote(
            moved.at[b, pl.ds(2 * (1 - xl), 2)], half.at[b], sx.at[d], rx.at[d], grp=g ^ 1
        )

    def along(d):
        b = (y + d) % 8
        return remote(mine.at[b], parts.at[d], sy.at[d], ry.at[d], grp=(g + 2 * d) % 16)

    for d in order:
        j = (y + d) % 8
        b = j // 4 * 4 + mapping[0, 8 * c + j] % 4
        moved[j] = dot(left[b], col_t[b]).reshape(4, BLK, BLK)
        across(d).start()

    first = (z == 0) & (c == 0)
    last = PAIRS.index((4, 4))

    @pl.when((z == 1) & (c == 0))
    def _():
        remote(moved.at[4, 0], extra, se, re, row=0).start()

    @pl.when(first)
    def _():
        for t, (i, j) in enumerate(PAIRS):
            if t == last:
                arrived(extra, se, re)
                src = extra
            else:
                src = moved.at[j, i]

            @pl.when(g != t)
            def _():
                remote(src, lparts.at[g], s1.at[t], r1.at[g], grp=t).start()

            @pl.when(g == t)
            def _():
                total[...] = src[...]

    for d in order:
        b = (y + d) % 8
        across(d).wait_recv()
        mine[b] = moved[b, pl.ds(2 * xl, 2)] + half[b]
        if d:
            along(d).start()

    @pl.when(first & (g < NPAIR))
    def _():
        for d in range(1, 16):
            arrived(lparts.at[(g + d) % 16], s1.at[0], r1.at[(g + d) % 16])
        acc = total[...]
        for d in range(1, 16):
            acc = acc + lparts[(g + d) % 16]
        total[...] = acc
        lead[g] = acc
        remote(total, lead.at[g], s2.at[0], r2, col=2).start()
        for d in FAR:
            remote(total, lead.at[g], s2.at[d], r2, row=(z + d) % 8).start()

    @pl.when((z == 0) & (c == 2) & (g < NPAIR))
    def _():
        arrived(lead.at[g], s2.at[0], r2)
        for d in FAR:
            remote(lead.at[g], lead.at[g], s2.at[d], r2, row=(z + d) % 8).start()

    acc = mine[y]
    for d in order[:-1]:
        along(d).wait_recv()
        acc = acc + parts[d]
    own[...] = acc

    for src_z, src_xl, start, count in COL_SOURCES:
        n = src_z * 2 + src_xl
        there = by_col.at[pl.ds(start, count)]
        src = own.at[pl.ds(0, count)]

        @pl.when((z == src_z) & (xl == src_xl))
        def _():
            for d in FAR:
                remote(src, there, sz.at[n, d], rz.at[n], row=(z + d) % 8).start()
            remote(src, there, sl.at[n], rl.at[n], grp=g ^ 1).start()
            by_col[start : start + count] = own[0:count]

    @pl.when((c == 0) & (y < NPAN))
    def _():
        remote(own, by_row.at[y], spx, rr.at[y], col=2).start()
        for d in FAR:
            remote(own, by_row.at[y], spy.at[d], rr.at[y], grp=(g + 2 * d) % 16).start()
        remote(own, by_row.at[y], sc.at[y], rcd.at[y], col=c ^ 1).start()
        by_row[y] = own[...]

    @pl.when((core == 0) & (g < NPAIR))
    def _():
        @pl.when(z != 0)
        def _():
            arrived(lead.at[g], s2.at[0], r2)
        for d in GRP_FAR:
            remote(lead.at[g], lead.at[g], s3.at[d], r3.at[g], grp=(g + d) % 16).start()
        remote(lead.at[g], lead.at[g], s4.at[0], r4.at[g], col=c ^ 1).start()

    @pl.when((c == 2) & (y < NPAN))
    def _():
        arrived(by_row.at[y], spx, rr.at[y])
        for d in FAR:
            remote(by_row.at[y], by_row.at[y], spy.at[d], rr.at[y], grp=(g + 2 * d) % 16).start()
        remote(by_row.at[y], by_row.at[y], sc.at[y], rcd.at[y], col=c ^ 1).start()

    for src_z, src_xl, start, count in COL_SOURCES:
        n = src_z * 2 + src_xl
        there = by_col.at[pl.ds(start, count)]

        @pl.when((z != src_z) & (xl == src_xl))
        def _():
            arrived(there, sz.at[n, 0], rz.at[n])
            remote(there, there, sl.at[n], rl.at[n], grp=g ^ 1).start()

    @pl.when(core == 0)
    def _():
        for k in range(NPAN):
            @pl.when(y != k)
            def _():
                arrived(by_row.at[k], spx, rr.at[k])
                remote(by_row.at[k], by_row.at[k], sc.at[k], rcd.at[k], col=c ^ 1).start()
        for d in range(1, 16):
            t = (g + d) % 16

            @pl.when(t < NPAIR)
            def _():
                arrived(lead.at[t], s3.at[0], r3.at[t])
                remote(lead.at[t], lead.at[t], s4.at[d], r4.at[t], col=c ^ 1).start()

    for src_z, src_xl, start, count in COL_SOURCES:
        n = src_z * 2 + src_xl

        @pl.when(xl != src_xl)
        def _():
            arrived(by_col.at[pl.ds(start, count)], sl.at[n], rl.at[n])

    @pl.when(core == 1)
    def _():
        for k in range(NPAN):
            arrived(by_row.at[k], sc.at[k], rcd.at[k])
        for t in range(NPAIR):
            arrived(lead.at[t], s4.at[0], r4.at[t])

    for slot in range(2):
        away = away_of(slot)
        for part in range(4):
            index = slot * 4 + part

            @pl.when(away < reach)
            def _():
                spread(index, col_t.at[index], send_r, up).wait_send()

            @pl.when((away > reach + 1) | (away == 0))
            def _():
                spread(index, col_t.at[index], send_l, down).wait_send()
    for d in order:
        across(d).wait_send()
        if d:
            along(d).wait_send()

    @pl.when((z == 1) & (c == 0))
    def _():
        remote(extra, extra, se, re, row=0).wait_send()

    @pl.when(first)
    def _():
        for t in range(NPAIR):
            @pl.when(g != t)
            def _():
                remote(extra, lparts.at[g], s1.at[t], r1.at[g], grp=t).wait_send()

        @pl.when(g < NPAIR)
        def _():
            remote(total, lead.at[g], s2.at[0], r2, col=2).wait_send()

    @pl.when((z == 0) & (core == 0) & (g < NPAIR))
    def _():
        for d in FAR:
            remote(total, lead.at[g], s2.at[d], r2, row=(z + d) % 8).wait_send()

    for src_z, src_xl, start, count in COL_SOURCES:
        n = src_z * 2 + src_xl
        there = by_col.at[pl.ds(start, count)]

        @pl.when(xl == src_xl)
        def _():
            @pl.when(z == src_z)
            def _():
                for d in FAR:
                    remote(there, there, sz.at[n, d], rz.at[n], row=(z + d) % 8).wait_send()
            remote(there, there, sl.at[n], rl.at[n], grp=g ^ 1).wait_send()

    @pl.when(core == 0)
    def _():
        @pl.when(y < NPAN)
        def _():
            @pl.when(c == 0)
            def _():
                remote(own, by_row.at[y], spx, rr.at[y], col=2).wait_send()
            for d in FAR:
                remote(own, by_row.at[y], spy.at[d], rr.at[y], grp=(g + 2 * d) % 16).wait_send()
        for k in range(NPAN):
            remote(own, by_row.at[k], sc.at[k], rcd.at[k], col=c ^ 1).wait_send()

        @pl.when(g < NPAIR)
        def _():
            for d in GRP_FAR:
                remote(total, lead.at[g], s3.at[d], r3.at[g], grp=(g + d) % 16).wait_send()
        for d in range(16):
            t = (g + d) % 16

            @pl.when(t < NPAIR)
            def _():
                remote(total, lead.at[t], s4.at[d], r4.at[t], col=c ^ 1).wait_send()


def gather(mapping, own_t, normal):
    dma = pltpu.SemaphoreType.DMA

    def buf(*shape):
        return pltpu.VMEM(shape, jnp.float32)

    return pl.pallas_call(
        gather_kernel,
        out_shape=(f32(NPAIR, BLK, BLK), f32(2, BLK, BLK), f32(NPAN, 2, BLK, BLK), f32(NPAN, BLK, BLK)),
        in_specs=[pl.BlockSpec(memory_space=pltpu.SMEM), VMEM, pl.BlockSpec(memory_space=pl.ANY)],
        out_specs=(VMEM,) * 4,
        scratch_shapes=[
            buf(4, BLK, 8 * BLK), buf(8, BLK, BLK), buf(8, 4 * BLK, BLK), buf(8, 4, BLK, BLK),
            buf(8, 2, BLK, BLK), buf(8, 2, BLK, BLK), buf(8, 2, BLK, BLK),
            buf(16, BLK, BLK), buf(BLK, BLK), buf(BLK, BLK),
            dma, dma((8,)), dma((8,)), dma((8,)), dma((8,)), dma((8,)), dma((8,)), dma((8,)),
            dma((16,)), dma((16,)), dma, dma, dma((8,)), dma, dma((16,)), dma((16,)), dma((16,)), dma((16,)),
            dma, dma((NPAN,)), dma((8,)), dma((NPAN,)), dma((NPAN,)), dma((3, 8)), dma((3,)), dma((3,)), dma((3,)),
        ],
        compiler_params=params(1),
    )(mapping, own_t, normal)


def factor_inverse(a):
    row_ids = lax.broadcasted_iota(jnp.int32, (BLK, BLK), 0)
    col_ids = lax.broadcasted_iota(jnp.int32, (BLK, BLK), 1)
    inv = jnp.where(row_ids == col_ids, 1.0, 0.0).astype(jnp.float32)
    done = []
    for start in range(0, BLK, STEP):
        rest = BLK - start
        cols = [jnp.broadcast_to(a[:, start + j : start + j + 1], (rest, BLK)) for j in range(STEP)]
        top_a, top_i = a[:STEP], inv[:STEP]
        rows_a, rows_i = [], []
        for j in range(STEP):
            scale = lax.rsqrt(cols[j][j : j + 1])
            cols[j] = cols[j] * scale
            row_a, row_i = top_a[j : j + 1] * scale, top_i[j : j + 1] * scale
            rows_a.append(row_a)
            rows_i.append(row_i)
            if j + 1 < STEP:
                low = cols[j][:STEP]
                top_a = top_a - low * row_a
                top_i = top_i - low * row_i
                for k in range(j + 1, STEP):
                    cols[k] = cols[k] - cols[j][k : k + 1] * cols[j]
        done.append(jnp.concatenate(rows_i, axis=0))
        if rest > STEP:
            a, inv = a[STEP:], inv[STEP:]
            for j in range(STEP):
                low = cols[j][STEP:]
                a = a - low * rows_a[j]
                inv = inv - low * rows_i[j]
    return jnp.concatenate(done, axis=0)


def mm(a, b):
    return jnp.dot(a, b, precision=HIGHEST, preferred_element_type=jnp.float32)


def mm_nt(a, b):
    return lax.dot_general(
        a, b, (((1,), (1,)), ((), ())), precision=HIGHEST, preferred_element_type=jnp.float32
    )


def eliminate_kernel(lead, by_row, by_col, own, out, square, upper, rows, cols):
    me = place()
    row_block = 4 * me["z"] + 2 * me["xl"]
    col_block = 8 * me["c"] + me["y"]
    for t, (i, j) in enumerate(PAIRS):
        square[i, j] = lead[t]
    rows[...] = by_row[...]
    cols[...] = by_col[...]
    out[...] = own[...]

    def panel(k, carry):
        inverse = factor_inverse(square[k, k])
        col_factor = mm(inverse, cols[k])
        row_factor = mm_nt(rows[k].reshape(2 * BLK, BLK), inverse)
        which = row_block + lax.broadcasted_iota(jnp.int32, (2 * BLK, BLK), 0) // BLK
        row_factor = jnp.where(which >= k, row_factor, 0.0)

        def solve(j, carry):
            upper[j] = mm(inverse, square[k, j])
            return carry

        lax.fori_loop(k + 1, NPAN, solve, 0)

        def update(i, carry):
            flipped = upper[i].T

            def inner(j, carry):
                square[i, j] -= mm(flipped, upper[j])
                return carry

            lax.fori_loop(i, NPAN, inner, 0)
            cols[i] -= mm(flipped, col_factor)
            rows[i] -= mm(row_factor, upper[i]).reshape(2, BLK, BLK)
            return carry

        lax.fori_loop(k + 1, NPAN, update, 0)

        @pl.when(col_block >= NPAN)
        def _():
            out[...] -= mm(row_factor, col_factor).reshape(2, BLK, BLK)

        @pl.when(col_block == k)
        def _():
            out[...] = row_factor.reshape(2, BLK, BLK)

        return carry

    lax.fori_loop(0, NPAN, panel, 0)


def eliminate(lead, by_row, by_col, own):
    return pl.pallas_call(
        eliminate_kernel,
        out_shape=f32(2, BLK, BLK),
        in_specs=[VMEM] * 4,
        out_specs=VMEM,
        scratch_shapes=[
            pltpu.VMEM((NPAN, NPAN, BLK, BLK), jnp.float32),
            pltpu.VMEM((NPAN, BLK, BLK), jnp.float32),
            pltpu.VMEM((NPAN, 2, BLK, BLK), jnp.float32),
            pltpu.VMEM((NPAN, BLK, BLK), jnp.float32),
        ],
        compiler_params=pltpu.CompilerParams(vmem_limit_bytes=40 << 20),
    )(lead, by_row, by_col, own)


HOPS = {
    "R1": (0, 1), "R2": (0, 2), "R3": (0, 3), "R4": (0, 4), "L1": (0, -1), "L2": (0, -2), "L3": (0, -3),
    "P0": (1, 0), "RP1": (1, 1), "LP1": (1, -1), "LP2": (1, -2),
    "X2": (1, 2), "X3": (1, 3), "X4": (1, 4), "XL": (1, -3),
}
NAMES = list(HOPS)
ONWARD = {
    "own": (("P0", "x"), ("R1", "r"), ("L1", "l")),
    "P0": (("RP1", "r"), ("LP1", "l")),
    "R1": (("R2", "r"),),
    "L1": (("L2", "l"),),
    "R2": (("R3", "r"), ("X2", "x")),
    "L2": (("L3", "l"),),
    "LP1": (("LP2", "l"),),
    "R3": (("R4", "r"), ("X3", "x")),
    "L3": (("XL", "x"),),
    "R4": (("X4", "x"),),
    "RP1": (), "LP2": (), "X2": (), "XL": (), "X3": (), "X4": (),
}


def collect_kernel(own, out, send, recv):
    me = place()
    g, y, xl = me["g"], me["y"], me["xl"]
    to = {"x": g ^ 1, "r": (g + 2) % 16, "l": (g + 14) % 16}
    meet([{"grp": to["x"]}, {"grp": to["r"]}, {"grp": to["l"]}])

    def spot(x, steps, part):
        row = pl.multiple_of((x * 2 + part) * BLK, BLK)
        col = pl.multiple_of(((y - steps + 8) % 8) * BLK, BLK)
        return out.at[pl.ds(row, BLK), pl.ds(col, BLK)]

    def here(name, part):
        other, steps = HOPS[name]
        return spot(1 - xl if other else xl, steps, part)

    def hop(src_name, name, way, part):
        if src_name == "own":
            src, dst = own.at[part], spot(xl, 0, part)
        else:
            src = dst = here(src_name, part)
        n = NAMES.index(name)
        return remote(src, dst, send.at[n, part], recv.at[n, part], grp=to[way])

    for part in range(2):
        for name, way in ONWARD["own"]:
            hop("own", name, way, part).start()
        row = pl.multiple_of((xl * 2 + part) * BLK, BLK)
        out[pl.ds(row, BLK), pl.ds(pl.multiple_of(y * BLK, BLK), BLK)] = own[part]
    for src_name in list(ONWARD)[1:]:
        for part in range(2):
            n = NAMES.index(src_name)
            arrived(here(src_name, part), send.at[n, part], recv.at[n, part])
            for name, way in ONWARD[src_name]:
                hop(src_name, name, way, part).start()
    for src_name in ONWARD:
        for name, way in ONWARD[src_name]:
            for part in range(2):
                hop(src_name, name, way, part).wait_send()


def collect(own):
    dma = pltpu.SemaphoreType.DMA
    return pl.pallas_call(
        collect_kernel,
        out_shape=f32(4 * BLK, 8 * BLK),
        in_specs=[VMEM],
        out_specs=VMEM,
        scratch_shapes=[dma((15, 2))] * 2,
        compiler_params=params(2),
    )(own)


def on_device(normals, transforms, block_map):
    lead, own, by_row, by_col = gather(block_map, transforms[0], normals.reshape(4, BLK, 8 * BLK))
    return collect(eliminate(lead, by_row, by_col, own))


def solution(mesh):
    return jax.shard_map(
        on_device,
        mesh=mesh,
        in_specs=(P("grp", "row", "col"), P("grp", "row", None, None), P("grp", None)),
        out_specs=P("row", "col"),
        check_vma=False,
    )
```

```python
import functools

import jax
import jax.numpy as jnp
from jax import lax
from jax.experimental import pallas as pl
from jax.experimental.pallas import tpu as pltpu
from jax.sharding import PartitionSpec as P

BLK = 128
NPAN = 5
STEP = 8
MESH = pl.DeviceIdType.MESH
HIGHEST = lax.Precision.HIGHEST
VMEM = pl.BlockSpec(memory_space=pltpu.VMEM)
PAIRS = [(i, j) for i in range(NPAN) for j in range(i, NPAN)]
NPAIR = len(PAIRS)


def f32(*shape):
    return jax.ShapeDtypeStruct(shape, jnp.float32)


def place():
    grp = lax.axis_index("grp")
    col = lax.axis_index("col")
    return dict(
        g=grp, y=grp // 2, xl=grp % 2, z=lax.axis_index("row"), c=col, xh=col // 2, core=col % 2
    )


def remote(src, dst, send, recv, **where):
    return pltpu.make_async_remote_copy(
        src_ref=src, dst_ref=dst, send_sem=send, recv_sem=recv, device_id=where, device_id_type=MESH
    )


def arrived(dst, send, recv):
    remote(dst, dst, send, recv, grp=lax.axis_index("grp")).wait_recv()


def meet(partners):
    barrier = pltpu.get_barrier_semaphore()
    for where in partners:
        pl.semaphore_signal(barrier, inc=1, device_id=where, device_id_type=MESH)
    pl.semaphore_wait(barrier, len(partners))


def params(ident):
    return pltpu.CompilerParams(collective_id=ident, has_side_effects=True, vmem_limit_bytes=40 << 20)


FAR = (4, 3, 5, 2, 6, 1, 7)
GRP_FAR = (8, 7, 9, 6, 10, 5, 11, 4, 12, 3, 13, 2, 14, 1, 15)
COL_SOURCES = ((0, 0, 0, 2), (0, 1, 2, 2), (1, 0, 4, 1))


def dot(a, b):
    return jnp.dot(a, b, precision=HIGHEST, preferred_element_type=jnp.float32)


def factor_inverse(a):
    row_ids = lax.broadcasted_iota(jnp.int32, (BLK, BLK), 0)
    col_ids = lax.broadcasted_iota(jnp.int32, (BLK, BLK), 1)
    inv = jnp.where(row_ids == col_ids, 1.0, 0.0).astype(jnp.float32)
    done = []
    for start in range(0, BLK, STEP):
        rest = BLK - start
        cols = [jnp.broadcast_to(a[:, start + j : start + j + 1], (rest, BLK)) for j in range(STEP)]
        top_a, top_i = a[:STEP], inv[:STEP]
        rows_a, rows_i = [], []
        for j in range(STEP):
            scale = lax.rsqrt(cols[j][j : j + 1])
            cols[j] = cols[j] * scale
            row_a, row_i = top_a[j : j + 1] * scale, top_i[j : j + 1] * scale
            rows_a.append(row_a)
            rows_i.append(row_i)
            if j + 1 < STEP:
                low = cols[j][:STEP]
                top_a = top_a - low * row_a
                top_i = top_i - low * row_i
                for k in range(j + 1, STEP):
                    cols[k] = cols[k] - cols[j][k : k + 1] * cols[j]
        done.append(jnp.concatenate(rows_i, axis=0))
        if rest > STEP:
            a, inv = a[STEP:], inv[STEP:]
            for j in range(STEP):
                low = cols[j][STEP:]
                a = a - low * rows_a[j]
                inv = inv - low * rows_i[j]
    return jnp.concatenate(done, axis=0)


def dot_nt(a, b):
    return lax.dot_general(
        a, b, (((1,), (1,)), ((), ())), precision=HIGHEST, preferred_element_type=jnp.float32
    )


HOPS = {
    "R1": (0, 1), "R2": (0, 2), "R3": (0, 3), "R4": (0, 4), "L1": (0, -1), "L2": (0, -2), "L3": (0, -3),
    "P0": (1, 0), "RP1": (1, 1), "LP1": (1, -1), "LP2": (1, -2),
    "X2": (1, 2), "X3": (1, 3), "X4": (1, 4), "XL": (1, -3),
}
NAMES = list(HOPS)
ONWARD = {
    "own": (("P0", "x"), ("R1", "r"), ("L1", "l")),
    "P0": (("RP1", "r"), ("LP1", "l")),
    "R1": (("R2", "r"),),
    "L1": (("L2", "l"),),
    "R2": (("R3", "r"), ("X2", "x")),
    "L2": (("L3", "l"),),
    "LP1": (("LP2", "l"),),
    "R3": (("R4", "r"), ("X3", "x")),
    "L3": (("XL", "x"),),
    "R4": (("X4", "x"),),
    "RP1": (), "LP2": (), "X2": (), "XL": (), "X3": (), "X4": (),
}


def whole_kernel(
    mapping, own_t_hbm, normal_hbm, out,
    lead, own, by_row, by_col, own_t, normal, col_t, left, moved, half, mine, parts, lparts, extra, total,
    square, upper, inverse, rows, cols, piece, sem_t,
    sem, send_r, send_l, recv, sx, rx, sy, ry,
    s1, r1, se, re, s2, r2, s3, r3, s4, r4, spx, rr, spy, sc, rcd, sz, rz, sl, rl,
    send6, recv6,
):
    me = place()
    g, y, xl, z, c, core = me["g"], me["y"], me["xl"], me["z"], me["c"], me["core"]
    fetch_t = pltpu.make_async_copy(own_t_hbm, own_t, sem_t)
    fetch_t.start()
    fetch = pltpu.make_async_copy(normal_hbm, normal, sem)
    fetch.start()
    meet(
        [{"grp": (g + d) % 16} for d in range(1, 16)]
        + [{"row": (z + d) % 8} for d in range(1, 8)]
        + [{"col": c ^ 1}, {"col": c ^ 2}]
    )

    fetch_t.wait()

    up, down = (z + 1) % 8, (z + 7) % 8
    reach = 4 - core

    def away_of(slot):
        return (z - (2 * c + slot) + 8) % 8

    def spread(index, src, sends, to):
        return remote(src, col_t.at[index], sends.at[index], recv.at[index], row=to)

    for slot in range(2):
        @pl.when(away_of(slot) == 0)
        def _():
            for part in range(4):
                index = slot * 4 + part
                spread(index, own_t.at[part], send_r, up).start()
                spread(index, own_t.at[part], send_l, down).start()
                col_t[index] = own_t[part]

    fetch.wait()
    for i in range(4):
        block = mapping[0, 4 * z + i] % 4
        turned = dot(own_t[block].T, normal[block])
        for b in range(8):
            left[b, i * BLK : (i + 1) * BLK, :] = turned[:, b * BLK : (b + 1) * BLK]

    rising = (away_of(1) <= reach).astype(jnp.int32)
    for part in range(4):
        for turn in range(2):
            slot = (rising + turn) % 2
            index = slot * 4 + part
            away = away_of(slot)

            @pl.when(away != 0)
            def _():
                arrived(col_t.at[index], send_r.at[index], recv.at[index])

            @pl.when((away > 0) & (away < reach))
            def _():
                spread(index, col_t.at[index], send_r, up).start()

            @pl.when(away > reach + 1)
            def _():
                spread(index, col_t.at[index], send_l, down).start()

    first = (z == 0) & (c == 0)
    order = (4, 1, 7, 2, 6, 3, 5, 0)

    def across(d):
        b = (y + d) % 8
        return remote(
            moved.at[b, pl.ds(2 * (1 - xl), 2)], half.at[b], sx.at[d], rx.at[d], grp=g ^ 1
        )

    def along(d):
        b = (y + d) % 8
        return remote(mine.at[b], parts.at[d], sy.at[d], ry.at[d], grp=(g + 2 * d) % 16)

    for d in order:
        j = (y + d) % 8
        b = j // 4 * 4 + mapping[0, 8 * c + j] % 4
        moved[j] = dot(left[b], col_t[b]).reshape(4, BLK, BLK)

        @pl.when(jnp.logical_not(first))
        def _():
            across(d).start()

    last = PAIRS.index((4, 4))

    @pl.when((z == 1) & (c == 0))
    def _():
        remote(moved.at[4, 0], extra, se, re, row=0).start()

    @pl.when(first)
    def _():
        for t, (i, j) in enumerate(PAIRS):
            if t == last:
                arrived(extra, se, re)
                src = extra
            else:
                src = moved.at[j, i]

            @pl.when(g != t)
            def _():
                remote(src, lparts.at[g], s1.at[t], r1.at[g], grp=t).start()

            @pl.when(g == t)
            def _():
                total[...] = src[...]

    @pl.when(first)
    def _():
        for d in order:
            across(d).start()

    @pl.when(first & (g < NPAIR))
    def _():
        for d in range(1, 16):
            arrived(lparts.at[(g + d) % 16], s1.at[0], r1.at[(g + d) % 16])
        acc = total[...]
        for d in range(1, 16):
            acc = acc + lparts[(g + d) % 16]
        total[...] = acc
        lead[g] = acc
        remote(total, lead.at[g], s2.at[0], r2, col=2).start()
        for d in FAR:
            remote(total, lead.at[g], s2.at[d], r2, row=(z + d) % 8).start()

    def among_members():
        for d in GRP_FAR:
            remote(lead.at[g], lead.at[g], s3.at[d], r3.at[g], grp=(g + d) % 16).start()
        remote(lead.at[g], lead.at[g], s4.at[0], r4.at[g], col=c ^ 1).start()

    @pl.when(first & (g < NPAIR))
    def _():
        among_members()

    for turn, d in enumerate(order):
        b = (y + d) % 8
        across(d).wait_recv()
        mine[b] = moved[b, pl.ds(2 * xl, 2)] + half[b]
        if d:
            along(d).start()
        if turn == 1:
            @pl.when((z != 0) & (c == 0) & (g < NPAIR))
            def _():
                arrived(lead.at[g], s2.at[0], r2)
                among_members()
        if turn == 2:
            @pl.when((z == 0) & (c == 2) & (g < NPAIR))
            def _():
                arrived(lead.at[g], s2.at[0], r2)
                for d2 in FAR:
                    remote(lead.at[g], lead.at[g], s2.at[d2], r2, row=(z + d2) % 8).start()
                among_members()
        if turn == 4:
            @pl.when((z != 0) & (c == 2) & (g < NPAIR))
            def _():
                arrived(lead.at[g], s2.at[0], r2)
                among_members()

    acc = mine[y]
    for d in order[:-1]:
        along(d).wait_recv()
        acc = acc + parts[d]
    own[...] = acc

    for src_z, src_xl, start, count in COL_SOURCES:
        n = src_z * 2 + src_xl
        there = by_col.at[pl.ds(start, count)]
        src = own.at[pl.ds(0, count)]

        @pl.when((z == src_z) & (xl == src_xl))
        def _():
            for d in FAR:
                remote(src, there, sz.at[n, d], rz.at[n], row=(z + d) % 8).start()
            remote(src, there, sl.at[n], rl.at[n], grp=g ^ 1).start()
            by_col[start : start + count] = own[0:count]

    @pl.when((c == 0) & (y < NPAN))
    def _():
        remote(own, by_row.at[y], spx, rr.at[y], col=2).start()
        for d in FAR:
            remote(own, by_row.at[y], spy.at[d], rr.at[y], grp=(g + 2 * d) % 16).start()
        remote(own, by_row.at[y], sc.at[y], rcd.at[y], col=c ^ 1).start()
        by_row[y] = own[...]

    @pl.when(core == 0)
    def _():
        for d in range(1, 16):
            t = (g + d) % 16

            @pl.when(t < NPAIR)
            def _():
                arrived(lead.at[t], s3.at[0], r3.at[t])
                remote(lead.at[t], lead.at[t], s4.at[d], r4.at[t], col=c ^ 1).start()

    @pl.when(core == 1)
    def _():
        for t in range(NPAIR):
            arrived(lead.at[t], s4.at[0], r4.at[t])

    for t, (i, j) in enumerate(PAIRS):
        square[i * BLK : (i + 1) * BLK, j * BLK : (j + 1) * BLK] = lead[t]

    def factor(k):
        low, high = k * BLK, (k + 1) * BLK
        inverse[k] = factor_inverse(square[low:high, low:high])
        if k + 1 < NPAN:
            across_panel = dot(inverse[k], square[low:high, high:])
            upper[low:high, high:] = across_panel
            square[high:, high:] -= dot(across_panel.T, across_panel)

    def rows_to_other_core(sources):
        @pl.when(sources)
        def _():
            for k in range(NPAN):
                @pl.when(y != k)
                def _():
                    arrived(by_row.at[k], spx, rr.at[k])
                    remote(by_row.at[k], by_row.at[k], sc.at[k], rcd.at[k], col=c ^ 1).start()

    factor(0)

    @pl.when((c == 2) & (y < NPAN))
    def _():
        arrived(by_row.at[y], spx, rr.at[y])
        for d in FAR:
            remote(by_row.at[y], by_row.at[y], spy.at[d], rr.at[y], grp=(g + 2 * d) % 16).start()
        remote(by_row.at[y], by_row.at[y], sc.at[y], rcd.at[y], col=c ^ 1).start()

    factor(1)
    factor(2)
    for src_z, src_xl, start, count in COL_SOURCES:
        n = src_z * 2 + src_xl
        there = by_col.at[pl.ds(start, count)]

        @pl.when((z != src_z) & (xl == src_xl))
        def _():
            arrived(there, sz.at[n, 0], rz.at[n])
            remote(there, there, sl.at[n], rl.at[n], grp=g ^ 1).start()

    factor(3)
    rows_to_other_core(c == 0)
    factor(4)
    rows_to_other_core(c == 2)
    for src_z, src_xl, start, count in COL_SOURCES:
        n = src_z * 2 + src_xl

        @pl.when(xl != src_xl)
        def _():
            arrived(by_col.at[pl.ds(start, count)], sl.at[n], rl.at[n])

    @pl.when(core == 1)
    def _():
        for k in range(NPAN):
            arrived(by_row.at[k], sc.at[k], rcd.at[k])

    row_block = 4 * z + 2 * xl
    col_block = 8 * c + y
    which = row_block + lax.broadcasted_iota(jnp.int32, (2 * BLK, BLK), 0) // BLK
    for k in range(NPAN):
        rows[:, k * BLK : (k + 1) * BLK] = by_row[k].reshape(2 * BLK, BLK)
    cols[...] = by_col[...].reshape(NPAN * BLK, BLK)
    panel_piece = jnp.zeros((2 * BLK, BLK), jnp.float32)
    for k in range(NPAN):
        low, high = k * BLK, (k + 1) * BLK
        col_factor = dot(inverse[k], cols[low:high])
        cols[low:high] = col_factor
        row_factor = jnp.where(which >= k, dot_nt(rows[:, low:high], inverse[k]), 0.0)
        rows[:, low:high] = row_factor
        panel_piece = jnp.where(col_block == k, row_factor, panel_piece)
        if k + 1 < NPAN:
            across_panel = upper[low:high, high:]
            cols[high:] -= dot(across_panel.T, col_factor)
            rows[:, high:] -= dot(row_factor, across_panel)
    rest = own[...].reshape(2 * BLK, BLK) - dot(rows[...], cols[...])
    piece[...] = jnp.where(col_block < NPAN, panel_piece, rest).reshape(2, BLK, BLK)

    to = {"x": g ^ 1, "r": (g + 2) % 16, "l": (g + 14) % 16}

    def spot(x, steps, part):
        row = pl.multiple_of((x * 2 + part) * BLK, BLK)
        col = pl.multiple_of(((y - steps + 8) % 8) * BLK, BLK)
        return out.at[pl.ds(row, BLK), pl.ds(col, BLK)]

    def here(name, part):
        other, steps = HOPS[name]
        return spot(1 - xl if other else xl, steps, part)

    def hop(src_name, name, way, part):
        if src_name == "own":
            src, dst = piece.at[part], spot(xl, 0, part)
        else:
            src = dst = here(src_name, part)
        n = NAMES.index(name)
        return remote(src, dst, send6.at[n, part], recv6.at[n, part], grp=to[way])

    for part in range(2):
        for name, way in ONWARD["own"]:
            hop("own", name, way, part).start()
        row = pl.multiple_of((xl * 2 + part) * BLK, BLK)
        out[pl.ds(row, BLK), pl.ds(pl.multiple_of(y * BLK, BLK), BLK)] = piece[part]
    for src_name in list(ONWARD)[1:]:
        for part in range(2):
            n = NAMES.index(src_name)
            arrived(here(src_name, part), send6.at[n, part], recv6.at[n, part])
            for name, way in ONWARD[src_name]:
                hop(src_name, name, way, part).start()
    for src_name in ONWARD:
        for name, way in ONWARD[src_name]:
            for part in range(2):
                hop(src_name, name, way, part).wait_send()

    for slot in range(2):
        away = away_of(slot)
        for part in range(4):
            index = slot * 4 + part

            @pl.when(away < reach)
            def _():
                spread(index, col_t.at[index], send_r, up).wait_send()

            @pl.when((away > reach + 1) | (away == 0))
            def _():
                spread(index, col_t.at[index], send_l, down).wait_send()
    for d in order:
        across(d).wait_send()
        if d:
            along(d).wait_send()

    @pl.when((z == 1) & (c == 0))
    def _():
        remote(extra, extra, se, re, row=0).wait_send()

    @pl.when(first)
    def _():
        for t in range(NPAIR):
            @pl.when(g != t)
            def _():
                remote(extra, lparts.at[g], s1.at[t], r1.at[g], grp=t).wait_send()

        @pl.when(g < NPAIR)
        def _():
            remote(total, lead.at[g], s2.at[0], r2, col=2).wait_send()

    @pl.when((z == 0) & (core == 0) & (g < NPAIR))
    def _():
        for d in FAR:
            remote(total, lead.at[g], s2.at[d], r2, row=(z + d) % 8).wait_send()

    for src_z, src_xl, start, count in COL_SOURCES:
        n = src_z * 2 + src_xl
        there = by_col.at[pl.ds(start, count)]

        @pl.when(xl == src_xl)
        def _():
            @pl.when(z == src_z)
            def _():
                for d in FAR:
                    remote(there, there, sz.at[n, d], rz.at[n], row=(z + d) % 8).wait_send()
            remote(there, there, sl.at[n], rl.at[n], grp=g ^ 1).wait_send()

    @pl.when(core == 0)
    def _():
        @pl.when(y < NPAN)
        def _():
            @pl.when(c == 0)
            def _():
                remote(own, by_row.at[y], spx, rr.at[y], col=2).wait_send()
            for d in FAR:
                remote(own, by_row.at[y], spy.at[d], rr.at[y], grp=(g + 2 * d) % 16).wait_send()
        for k in range(NPAN):
            remote(own, by_row.at[k], sc.at[k], rcd.at[k], col=c ^ 1).wait_send()

        @pl.when(g < NPAIR)
        def _():
            for d in GRP_FAR:
                remote(total, lead.at[g], s3.at[d], r3.at[g], grp=(g + d) % 16).wait_send()
        for d in range(16):
            t = (g + d) % 16

            @pl.when(t < NPAIR)
            def _():
                remote(total, lead.at[t], s4.at[d], r4.at[t], col=c ^ 1).wait_send()


def whole(mapping, own_t, normal):
    dma = pltpu.SemaphoreType.DMA

    def buf(*shape):
        return pltpu.VMEM(shape, jnp.float32)

    order = NPAN * BLK
    hbm = pl.BlockSpec(memory_space=pltpu.HBM)
    return pl.pallas_call(
        whole_kernel,
        out_shape=f32(4 * BLK, 8 * BLK),
        in_specs=[pl.BlockSpec(memory_space=pltpu.SMEM), hbm, hbm],
        out_specs=VMEM,
        scratch_shapes=[
            buf(NPAIR, BLK, BLK), buf(2, BLK, BLK), buf(NPAN, 2, BLK, BLK), buf(NPAN, BLK, BLK),
            buf(4, BLK, BLK), buf(4, BLK, 8 * BLK), buf(8, BLK, BLK), buf(8, 4 * BLK, BLK), buf(8, 4, BLK, BLK),
            buf(8, 2, BLK, BLK), buf(8, 2, BLK, BLK), buf(8, 2, BLK, BLK),
            buf(16, BLK, BLK), buf(BLK, BLK), buf(BLK, BLK),
            buf(order, order), buf(order, order), buf(NPAN, BLK, BLK), buf(2 * BLK, order), buf(order, BLK),
            buf(2, BLK, BLK),
            dma, dma, dma((8,)), dma((8,)), dma((8,)), dma((8,)), dma((8,)), dma((8,)), dma((8,)),
            dma((16,)), dma((16,)), dma, dma, dma((8,)), dma, dma((16,)), dma((16,)), dma((16,)), dma((16,)),
            dma, dma((NPAN,)), dma((8,)), dma((NPAN,)), dma((NPAN,)), dma((3, 8)), dma((3,)), dma((3,)), dma((3,)),
            dma((15, 2)), dma((15, 2)),
        ],
        compiler_params=params(1),
    )(mapping, own_t, normal)


def on_device(normals, transforms, block_map):
    return whole(block_map, transforms[0], normals.reshape(4, BLK, 8 * BLK))


def solution(mesh):
    return jax.shard_map(
        on_device,
        mesh=mesh,
        in_specs=(P("grp", "row", "col"), P("grp", "row", None, None), P("grp", None)),
        out_specs=P("row", "col"),
        check_vma=False,
    )
```

```python
import functools

import jax
import jax.numpy as jnp
from jax import lax
from jax.experimental import pallas as pl
from jax.experimental.pallas import tpu as pltpu
from jax.sharding import PartitionSpec as P

BLK = 128
NPAN = 5
STEP = 8
MESH = pl.DeviceIdType.MESH
HIGHEST = lax.Precision.HIGHEST
VMEM = pl.BlockSpec(memory_space=pltpu.VMEM)
PAIRS = [(i, j) for i in range(NPAN) for j in range(i, NPAN)]
NPAIR = len(PAIRS)


def f32(*shape):
    return jax.ShapeDtypeStruct(shape, jnp.float32)


def place():
    grp = lax.axis_index("grp")
    col = lax.axis_index("col")
    return dict(
        g=grp, y=grp // 2, xl=grp % 2, z=lax.axis_index("row"), c=col, xh=col // 2, core=col % 2
    )


def remote(src, dst, send, recv, **where):
    return pltpu.make_async_remote_copy(
        src_ref=src, dst_ref=dst, send_sem=send, recv_sem=recv, device_id=where, device_id_type=MESH
    )


def arrived(dst, send, recv):
    remote(dst, dst, send, recv, grp=lax.axis_index("grp")).wait_recv()


def meet(partners):
    barrier = pltpu.get_barrier_semaphore()
    for where in partners:
        pl.semaphore_signal(barrier, inc=1, device_id=where, device_id_type=MESH)
    pl.semaphore_wait(barrier, len(partners))


def params(ident):
    return pltpu.CompilerParams(collective_id=ident, has_side_effects=True, vmem_limit_bytes=53300000)


FAR = (4, 3, 5, 2, 6, 1, 7)
GRP_FAR = (8, 7, 9, 6, 10, 5, 11, 4, 12, 3, 13, 2, 14, 1, 15)
COL_SOURCES = ((0, 0, 0, 2), (0, 1, 2, 2), (1, 0, 4, 1))


def dot(a, b):
    return jnp.dot(a, b, precision=HIGHEST, preferred_element_type=jnp.float32)


def factor_inverse(a):
    row_ids = lax.broadcasted_iota(jnp.int32, (BLK, BLK), 0)
    col_ids = lax.broadcasted_iota(jnp.int32, (BLK, BLK), 1)
    inv = jnp.where(row_ids == col_ids, 1.0, 0.0).astype(jnp.float32)
    done = []
    for start in range(0, BLK, STEP):
        rest = BLK - start
        cols = [jnp.broadcast_to(a[:, start + j : start + j + 1], (rest, BLK)) for j in range(STEP)]
        top_a, top_i = a[:STEP], inv[:STEP]
        rows_a, rows_i = [], []
        for j in range(STEP):
            scale = lax.rsqrt(cols[j][j : j + 1])
            cols[j] = cols[j] * scale
            row_a, row_i = top_a[j : j + 1] * scale, top_i[j : j + 1] * scale
            rows_a.append(row_a)
            rows_i.append(row_i)
            if j + 1 < STEP:
                low = cols[j][:STEP]
                top_a = top_a - low * row_a
                top_i = top_i - low * row_i
                for k in range(j + 1, STEP):
                    cols[k] = cols[k] - cols[j][k : k + 1] * cols[j]
        done.append(jnp.concatenate(rows_i, axis=0))
        if rest > STEP:
            a, inv = a[STEP:], inv[STEP:]
            for j in range(STEP):
                low = cols[j][STEP:]
                a = a - low * rows_a[j]
                inv = inv - low * rows_i[j]
    return jnp.concatenate(done, axis=0)


def dot_nt(a, b):
    return lax.dot_general(
        a, b, (((1,), (1,)), ((), ())), precision=HIGHEST, preferred_element_type=jnp.float32
    )


HOPS = {
    "R1": (0, 1), "R2": (0, 2), "R3": (0, 3), "R4": (0, 4), "L1": (0, -1), "L2": (0, -2), "L3": (0, -3),
    "P0": (1, 0), "RP1": (1, 1), "LP1": (1, -1), "LP2": (1, -2),
    "X2": (1, 2), "X3": (1, 3), "X4": (1, 4), "XL": (1, -3),
}
NAMES = list(HOPS)
ONWARD = {
    "own": (("P0", "x"), ("R1", "r"), ("L1", "l")),
    "P0": (("RP1", "r"), ("LP1", "l")),
    "R1": (("R2", "r"),),
    "L1": (("L2", "l"),),
    "R2": (("R3", "r"), ("X2", "x")),
    "L2": (("L3", "l"),),
    "LP1": (("LP2", "l"),),
    "R3": (("R4", "r"), ("X3", "x")),
    "L3": (("XL", "x"),),
    "R4": (("X4", "x"),),
    "RP1": (), "LP2": (), "X2": (), "XL": (), "X3": (), "X4": (),
}


def whole_kernel(
    mapping, own_t_hbm, normal_hbm, out,
    lead, own, by_row, by_col, own_t, normal, col_t, left, moved, half, mine, parts, lparts, extra, total,
    square, upper, inverse, rows, cols, piece, sem_t,
    sem, send_r, send_l, recv, sx, rx, sy, ry,
    s1, r1, se, re, s2, r2, s3, r3, s4, r4, spx, rr, spy, sc, rcd, sz, rz, sl, rl,
    send6, recv6,
):
    me = place()
    g, y, xl, z, c, core = me["g"], me["y"], me["xl"], me["z"], me["c"], me["core"]
    fetch_t = pltpu.make_async_copy(own_t_hbm, own_t, sem_t)
    fetch_t.start()
    fetch = pltpu.make_async_copy(normal_hbm, normal, sem)
    fetch.start()
    meet(
        [{"grp": (g + d) % 16} for d in range(1, 16)]
        + [{"row": (z + d) % 8} for d in range(1, 8)]
        + [{"col": c ^ 1}]
        + [{"row": (z + d) % 8, "col": c ^ 2} for d in range(8)]
    )

    fetch_t.wait()

    up, down = (z + 1) % 8, (z + 7) % 8
    reach = 4 - core

    def away_of(slot):
        return (z - (2 * c + slot) + 8) % 8

    def spread(index, src, sends, to):
        return remote(src, col_t.at[index], sends.at[index], recv.at[index], row=to)

    for slot in range(2):
        @pl.when(away_of(slot) == 0)
        def _():
            for part in range(4):
                index = slot * 4 + part
                spread(index, own_t.at[part], send_r, up).start()
                spread(index, own_t.at[part], send_l, down).start()
                col_t[index] = own_t[part]

    fetch.wait()
    for i in range(4):
        block = mapping[0, 4 * z + i] % 4
        turned = dot(own_t[block].T, normal[block])
        for b in range(8):
            left[b, i * BLK : (i + 1) * BLK, :] = turned[:, b * BLK : (b + 1) * BLK]

    rising = (away_of(1) <= reach).astype(jnp.int32)
    for part in range(4):
        for turn in range(2):
            slot = (rising + turn) % 2
            index = slot * 4 + part
            away = away_of(slot)

            @pl.when(away != 0)
            def _():
                arrived(col_t.at[index], send_r.at[index], recv.at[index])

            @pl.when((away > 0) & (away < reach))
            def _():
                spread(index, col_t.at[index], send_r, up).start()

            @pl.when(away > reach + 1)
            def _():
                spread(index, col_t.at[index], send_l, down).start()

    first = (z == 0) & (c == 0)
    order = (4, 1, 7, 2, 6, 3, 5, 0)

    def across(d):
        b = (y + d) % 8
        return remote(
            moved.at[b, pl.ds(2 * (1 - xl), 2)], half.at[b], sx.at[d], rx.at[d], grp=g ^ 1
        )

    def along(d):
        b = (y + d) % 8
        return remote(mine.at[b], parts.at[d], sy.at[d], ry.at[d], grp=(g + 2 * d) % 16)

    def combine(j):
        b = j // 4 * 4 + mapping[0, 8 * c + j] % 4
        moved[j] = dot(left[b], col_t[b]).reshape(4, BLK, BLK)

    last = PAIRS.index((4, 4))

    @pl.when(jnp.logical_not(first))
    def _():
        @pl.when((z == 1) & (c == 0))
        def _():
            combine(4)
            remote(moved.at[4, 0], extra, se, re, row=0).start()

        for d in order:
            j = (y + d) % 8

            @pl.when(jnp.logical_not((z == 1) & (c == 0) & (j == 4)))
            def _():
                combine(j)

            across(d).start()

    @pl.when(first)
    def _():
        for j in range(NPAN):
            combine(j)
        for t, (i, j) in enumerate(PAIRS):
            if t == last:
                arrived(extra, se, re)
                src = extra
            else:
                src = moved.at[j, i]

            @pl.when(g != t)
            def _():
                remote(src, lparts.at[g], s1.at[t], r1.at[g], grp=t).start()

            @pl.when(g == t)
            def _():
                total[...] = src[...]

        for j in range(NPAN, 8):
            combine(j)
        for d in order:
            across(d).start()

    def among_members():
        for d in GRP_FAR:
            remote(lead.at[g], lead.at[g], s3.at[d], r3.at[g], grp=(g + d) % 16).start()
        remote(lead.at[g], lead.at[g], s4.at[0], r4.at[g], col=c ^ 1).start()

    def to_rows(d):
        return (
            remote(total, lead.at[g], s2.at[d], r2, row=(z + d) % 8, col=2),
            remote(total, lead.at[g], s2.at[8 + d], r2, row=(z + d) % 8, col=0),
        )

    @pl.when(first & (g < NPAIR))
    def _():
        for d in range(1, 16):
            arrived(lparts.at[(g + d) % 16], s1.at[0], r1.at[(g + d) % 16])
        acc = total[...]
        for d in range(1, 16):
            acc = acc + lparts[(g + d) % 16]
        total[...] = acc
        lead[g] = acc
        for d in FAR + (0,):
            for copy in to_rows(d)[: 2 if d else 1]:
                copy.start()
        among_members()

    for turn, d in enumerate(order):
        b = (y + d) % 8
        across(d).wait_recv()
        mine[b] = moved[b, pl.ds(2 * xl, 2)] + half[b]
        if d:
            along(d).start()
        if turn == 5:
            @pl.when(jnp.logical_not(first) & (core == 0) & (g < NPAIR))
            def _():
                arrived(lead.at[g], s2.at[0], r2)
                among_members()

    acc = mine[y]
    for d in order[:-1]:
        along(d).wait_recv()
        acc = acc + parts[d]
    own[...] = acc

    for src_z, src_xl, start, count in COL_SOURCES:
        n = src_z * 2 + src_xl
        there = by_col.at[pl.ds(start, count)]
        src = own.at[pl.ds(0, count)]

        @pl.when((z == src_z) & (xl == src_xl))
        def _():
            for d in FAR:
                remote(src, there, sz.at[n, d], rz.at[n], row=(z + d) % 8).start()
            remote(src, there, sl.at[n], rl.at[n], grp=g ^ 1).start()
            by_col[start : start + count] = own[0:count]

    @pl.when((c == 0) & (y < NPAN))
    def _():
        remote(own, by_row.at[y], spx, rr.at[y], col=2).start()
        for d in FAR:
            remote(own, by_row.at[y], spy.at[d], rr.at[y], grp=(g + 2 * d) % 16).start()
        remote(own, by_row.at[y], sc.at[y], rcd.at[y], col=c ^ 1).start()
        by_row[y] = own[...]

    @pl.when(core == 0)
    def _():
        for d in range(1, 16):
            t = (g + d) % 16

            @pl.when(t < NPAIR)
            def _():
                arrived(lead.at[t], s3.at[0], r3.at[t])
                remote(lead.at[t], lead.at[t], s4.at[d], r4.at[t], col=c ^ 1).start()

    @pl.when(core == 1)
    def _():
        for t in range(NPAIR):
            arrived(lead.at[t], s4.at[0], r4.at[t])

    for t, (i, j) in enumerate(PAIRS):
        square[i * BLK : (i + 1) * BLK, j * BLK : (j + 1) * BLK] = lead[t]

    def factor(k):
        low, high = k * BLK, (k + 1) * BLK
        inverse[k] = factor_inverse(square[low:high, low:high])
        if k + 1 < NPAN:
            across_panel = dot(inverse[k], square[low:high, high:])
            upper[low:high, high:] = across_panel
            square[high:, high:] -= dot(across_panel.T, across_panel)

    factor(0)

    @pl.when((c == 2) & (y < NPAN))
    def _():
        arrived(by_row.at[y], spx, rr.at[y])
        for d in FAR:
            remote(by_row.at[y], by_row.at[y], spy.at[d], rr.at[y], grp=(g + 2 * d) % 16).start()
        remote(by_row.at[y], by_row.at[y], sc.at[y], rcd.at[y], col=c ^ 1).start()

    factor(1)
    factor(2)
    for src_z, src_xl, start, count in COL_SOURCES:
        n = src_z * 2 + src_xl
        there = by_col.at[pl.ds(start, count)]

        @pl.when((z != src_z) & (xl == src_xl))
        def _():
            arrived(there, sz.at[n, 0], rz.at[n])
            remote(there, there, sl.at[n], rl.at[n], grp=g ^ 1).start()

    factor(3)

    @pl.when(core == 0)
    def _():
        for k in range(NPAN):
            @pl.when(y != k)
            def _():
                arrived(by_row.at[k], spx, rr.at[k])
                remote(by_row.at[k], by_row.at[k], sc.at[k], rcd.at[k], col=c ^ 1).start()

    for src_z, src_xl, start, count in COL_SOURCES:
        n = src_z * 2 + src_xl

        @pl.when(xl != src_xl)
        def _():
            arrived(by_col.at[pl.ds(start, count)], sl.at[n], rl.at[n])

    @pl.when(core == 1)
    def _():
        for k in range(NPAN):
            arrived(by_row.at[k], sc.at[k], rcd.at[k])

    row_block = 4 * z + 2 * xl
    col_block = 8 * c + y
    which = row_block + lax.broadcasted_iota(jnp.int32, (2 * BLK, BLK), 0) // BLK
    for k in range(NPAN):
        rows[:, k * BLK : (k + 1) * BLK] = by_row[k].reshape(2 * BLK, BLK)
    cols[...] = by_col[...].reshape(NPAN * BLK, BLK)
    panel_piece = jnp.zeros((2 * BLK, BLK), jnp.float32)
    rest = own[...].reshape(2 * BLK, BLK)
    factor(4)
    for k in range(NPAN):
        low, high = k * BLK, (k + 1) * BLK
        col_factor = dot(inverse[k], cols[low:high])
        row_factor = jnp.where(which >= k, dot_nt(rows[:, low:high], inverse[k]), 0.0)
        panel_piece = jnp.where(col_block == k, row_factor, panel_piece)
        if k + 1 < NPAN:
            across_panel = upper[low:high, high:]
            cols[high:] -= dot(across_panel.T, col_factor)
            rows[:, high:] -= dot(row_factor, across_panel)
        rest = rest - dot(row_factor, col_factor)
    piece[...] = jnp.where(col_block < NPAN, panel_piece, rest).reshape(2, BLK, BLK)

    to = {"x": g ^ 1, "r": (g + 2) % 16, "l": (g + 14) % 16}

    def spot(x, steps, part):
        row = pl.multiple_of((x * 2 + part) * BLK, BLK)
        col = pl.multiple_of(((y - steps + 8) % 8) * BLK, BLK)
        return out.at[pl.ds(row, BLK), pl.ds(col, BLK)]

    def here(name, part):
        other, steps = HOPS[name]
        return spot(1 - xl if other else xl, steps, part)

    def hop(src_name, name, way, part):
        if src_name == "own":
            src, dst = piece.at[part], spot(xl, 0, part)
        else:
            src = dst = here(src_name, part)
        n = NAMES.index(name)
        return remote(src, dst, send6.at[n, part], recv6.at[n, part], grp=to[way])

    for part in range(2):
        for name, way in ONWARD["own"]:
            hop("own", name, way, part).start()
        row = pl.multiple_of((xl * 2 + part) * BLK, BLK)
        out[pl.ds(row, BLK), pl.ds(pl.multiple_of(y * BLK, BLK), BLK)] = piece[part]
    for src_name in list(ONWARD)[1:]:
        for part in range(2):
            n = NAMES.index(src_name)
            arrived(here(src_name, part), send6.at[n, part], recv6.at[n, part])
            for name, way in ONWARD[src_name]:
                hop(src_name, name, way, part).start()
    for src_name in ONWARD:
        for name, way in ONWARD[src_name]:
            for part in range(2):
                hop(src_name, name, way, part).wait_send()

    for slot in range(2):
        away = away_of(slot)
        for part in range(4):
            index = slot * 4 + part

            @pl.when(away < reach)
            def _():
                spread(index, col_t.at[index], send_r, up).wait_send()

            @pl.when((away > reach + 1) | (away == 0))
            def _():
                spread(index, col_t.at[index], send_l, down).wait_send()
    for d in order:
        across(d).wait_send()
        if d:
            along(d).wait_send()

    @pl.when((z == 1) & (c == 0))
    def _():
        remote(extra, extra, se, re, row=0).wait_send()

    @pl.when(first)
    def _():
        for t in range(NPAIR):
            @pl.when(g != t)
            def _():
                remote(extra, lparts.at[g], s1.at[t], r1.at[g], grp=t).wait_send()

        @pl.when(g < NPAIR)
        def _():
            for d in FAR + (0,):
                for copy in to_rows(d)[: 2 if d else 1]:
                    copy.wait_send()

    for src_z, src_xl, start, count in COL_SOURCES:
        n = src_z * 2 + src_xl
        there = by_col.at[pl.ds(start, count)]

        @pl.when(xl == src_xl)
        def _():
            @pl.when(z == src_z)
            def _():
                for d in FAR:
                    remote(there, there, sz.at[n, d], rz.at[n], row=(z + d) % 8).wait_send()
            remote(there, there, sl.at[n], rl.at[n], grp=g ^ 1).wait_send()

    @pl.when(core == 0)
    def _():
        @pl.when(y < NPAN)
        def _():
            @pl.when(c == 0)
            def _():
                remote(own, by_row.at[y], spx, rr.at[y], col=2).wait_send()
            for d in FAR:
                remote(own, by_row.at[y], spy.at[d], rr.at[y], grp=(g + 2 * d) % 16).wait_send()
        for k in range(NPAN):
            remote(own, by_row.at[k], sc.at[k], rcd.at[k], col=c ^ 1).wait_send()

        @pl.when(g < NPAIR)
        def _():
            for d in GRP_FAR:
                remote(total, lead.at[g], s3.at[d], r3.at[g], grp=(g + d) % 16).wait_send()
        for d in range(16):
            t = (g + d) % 16

            @pl.when(t < NPAIR)
            def _():
                remote(total, lead.at[t], s4.at[d], r4.at[t], col=c ^ 1).wait_send()


def whole(mapping, own_t, normal):
    dma = pltpu.SemaphoreType.DMA

    def buf(*shape):
        return pltpu.VMEM(shape, jnp.float32)

    order = NPAN * BLK
    hbm = pl.BlockSpec(memory_space=pltpu.HBM)
    return pl.pallas_call(
        whole_kernel,
        out_shape=f32(4 * BLK, 8 * BLK),
        in_specs=[pl.BlockSpec(memory_space=pltpu.SMEM), hbm, hbm],
        out_specs=VMEM,
        scratch_shapes=[
            buf(NPAIR, BLK, BLK), buf(2, BLK, BLK), buf(NPAN, 2, BLK, BLK), buf(NPAN, BLK, BLK),
            buf(4, BLK, BLK), buf(4, BLK, 8 * BLK), buf(8, BLK, BLK), buf(8, 4 * BLK, BLK), buf(8, 4, BLK, BLK),
            buf(8, 2, BLK, BLK), buf(8, 2, BLK, BLK), buf(8, 2, BLK, BLK),
            buf(16, BLK, BLK), buf(BLK, BLK), buf(BLK, BLK),
            buf(order, order), buf(order, order), buf(NPAN, BLK, BLK), buf(2 * BLK, order), buf(order, BLK),
            buf(2, BLK, BLK),
            dma, dma, dma((8,)), dma((8,)), dma((8,)), dma((8,)), dma((8,)), dma((8,)), dma((8,)),
            dma((16,)), dma((16,)), dma, dma, dma((16,)), dma, dma((16,)), dma((16,)), dma((16,)), dma((16,)),
            dma, dma((NPAN,)), dma((8,)), dma((NPAN,)), dma((NPAN,)), dma((3, 8)), dma((3,)), dma((3,)), dma((3,)),
            dma((15, 2)), dma((15, 2)),
        ],
        compiler_params=params(1),
    )(mapping, own_t, normal)


def on_device(normals, transforms, block_map):
    return whole(block_map, transforms[0], normals.reshape(4, BLK, 8 * BLK))


def solution(mesh):
    return jax.shard_map(
        on_device,
        mesh=mesh,
        in_specs=(P("grp", "row", "col"), P("grp", "row", None, None), P("grp", None)),
        out_specs=P("row", "col"),
        check_vma=False,
    )
```

```python
import functools

import jax
import jax.numpy as jnp
from jax import lax
from jax.experimental import pallas as pl
from jax.experimental.pallas import tpu as pltpu
from jax.sharding import PartitionSpec as P

BLK = 128
NPAN = 5
STEP = 8
MESH = pl.DeviceIdType.MESH
HIGHEST = lax.Precision.HIGHEST
VMEM = pl.BlockSpec(memory_space=pltpu.VMEM)
PAIRS = [(i, j) for i in range(NPAN) for j in range(i, NPAN)]
NPAIR = len(PAIRS)


def f32(*shape):
    return jax.ShapeDtypeStruct(shape, jnp.float32)


def place():
    grp = lax.axis_index("grp")
    col = lax.axis_index("col")
    return dict(
        g=grp, y=grp // 2, xl=grp % 2, z=lax.axis_index("row"), c=col, xh=col // 2, core=col % 2
    )


def remote(src, dst, send, recv, **where):
    return pltpu.make_async_remote_copy(
        src_ref=src, dst_ref=dst, send_sem=send, recv_sem=recv, device_id=where, device_id_type=MESH
    )


def arrived(dst, send, recv):
    remote(dst, dst, send, recv, grp=lax.axis_index("grp")).wait_recv()


def meet(partners):
    barrier = pltpu.get_barrier_semaphore()
    for where in partners:
        pl.semaphore_signal(barrier, inc=1, device_id=where, device_id_type=MESH)
    pl.semaphore_wait(barrier, len(partners))


def params(ident):
    return pltpu.CompilerParams(collective_id=ident, has_side_effects=True, vmem_limit_bytes=53300000)


FAR = (4, 3, 5, 2, 6, 1, 7)
GRP_FAR = (8, 7, 9, 6, 10, 5, 11, 4, 12, 3, 13, 2, 14, 1, 15)
COL_SOURCES = ((0, 0, 0, 2), (0, 1, 2, 2), (1, 0, 4, 1))


def dot(a, b):
    return jnp.dot(a, b, precision=HIGHEST, preferred_element_type=jnp.float32)


def factor_inverse(a):
    row_ids = lax.broadcasted_iota(jnp.int32, (BLK, BLK), 0)
    col_ids = lax.broadcasted_iota(jnp.int32, (BLK, BLK), 1)
    done = []
    for start in range(0, BLK, STEP):
        rest = BLK - start
        cols = [jnp.broadcast_to(a[:, start + j : start + j + 1], (rest, BLK)) for j in range(STEP)]
        here = (col_ids[start:] >= start) & (col_ids[start:] < start + STEP)
        unit = jnp.where(col_ids[start:] == row_ids[start:], 1.0, 0.0).astype(jnp.float32)
        a = jnp.where(here, unit, a)
        top = a[:STEP]
        rows = []
        for j in range(STEP):
            scale = lax.rsqrt(cols[j][j : j + 1])
            cols[j] = cols[j] * scale
            row = top[j : j + 1] * scale
            rows.append(row)
            if j + 1 < STEP:
                top = top - cols[j][:STEP] * row
                for k in range(j + 1, STEP):
                    cols[k] = cols[k] - cols[j][k : k + 1] * cols[j]
        done.append(jnp.concatenate(rows, axis=0))
        if rest > STEP:
            a = a[STEP:]
            for j in range(STEP):
                a = a - cols[j][STEP:] * rows[j]
    return jnp.where(col_ids <= row_ids, jnp.concatenate(done, axis=0), 0.0)


def dot_nt(a, b):
    return lax.dot_general(
        a, b, (((1,), (1,)), ((), ())), precision=HIGHEST, preferred_element_type=jnp.float32
    )


HOPS = {
    "R1": (0, 1), "R2": (0, 2), "R3": (0, 3), "R4": (0, 4), "L1": (0, -1), "L2": (0, -2), "L3": (0, -3),
    "P0": (1, 0), "RP1": (1, 1), "LP1": (1, -1), "LP2": (1, -2),
    "X2": (1, 2), "X3": (1, 3), "X4": (1, 4), "XL": (1, -3),
}
NAMES = list(HOPS)
ONWARD = {
    "own": (("P0", "x"), ("R1", "r"), ("L1", "l")),
    "P0": (("RP1", "r"), ("LP1", "l")),
    "R1": (("R2", "r"),),
    "L1": (("L2", "l"),),
    "R2": (("R3", "r"), ("X2", "x")),
    "L2": (("L3", "l"),),
    "LP1": (("LP2", "l"),),
    "R3": (("R4", "r"), ("X3", "x")),
    "L3": (("XL", "x"),),
    "R4": (("X4", "x"),),
    "RP1": (), "LP2": (), "X2": (), "XL": (), "X3": (), "X4": (),
}


def whole_kernel(
    mapping, own_t_hbm, normal_hbm, out,
    lead, own, by_row, by_col, own_t, normal, col_t, left, moved, half, mine, parts, lparts, lblk, lx, lsum, total,
    square, upper, inverse, rows, cols, piece, sem_t,
    sem, send_r, send_l, recv, sx, rx, sy, ry,
    s1, r1, se, re, s2, r2, s3, r3, s4, r4, spx, rr, spy, sc, rcd, sz, rz, sl, rl,
    send6, recv6, sl1, rl1,
):
    me = place()
    g, y, xl, z, c, core = me["g"], me["y"], me["xl"], me["z"], me["c"], me["core"]
    fetch_t = pltpu.make_async_copy(own_t_hbm, own_t, sem_t)
    fetch_t.start()
    fetch = pltpu.make_async_copy(normal_hbm, normal, sem)
    fetch.start()
    meet(
        [{"grp": (g + d) % 16} for d in range(1, 16)]
        + [{"row": (z + d) % 8} for d in range(1, 8)]
        + [{"col": c ^ 1}]
        + [{"row": (z + d) % 8, "col": c ^ 2} for d in range(8)]
    )

    fetch_t.wait()

    up, down = (z + 1) % 8, (z + 7) % 8
    reach = 4 - core

    def away_of(slot):
        return (z - (2 * c + slot) + 8) % 8

    def spread(index, src, sends, to):
        return remote(src, col_t.at[index], sends.at[index], recv.at[index], row=to)

    for slot in range(2):
        @pl.when(away_of(slot) == 0)
        def _():
            for part in range(4):
                index = slot * 4 + part
                spread(index, own_t.at[part], send_r, up).start()
                spread(index, own_t.at[part], send_l, down).start()
                col_t[index] = own_t[part]

    fetch.wait()
    for i in range(4):
        block = mapping[0, 4 * z + i] % 4
        turned = dot(own_t[block].T, normal[block])
        for b in range(8):
            left[b, i * BLK : (i + 1) * BLK, :] = turned[:, b * BLK : (b + 1) * BLK]

    rising = (away_of(1) <= reach).astype(jnp.int32)
    for part in range(4):
        for turn in range(2):
            slot = (rising + turn) % 2
            index = slot * 4 + part
            away = away_of(slot)

            @pl.when(away != 0)
            def _():
                arrived(col_t.at[index], send_r.at[index], recv.at[index])

            @pl.when((away > 0) & (away < reach))
            def _():
                spread(index, col_t.at[index], send_r, up).start()

            @pl.when(away > reach + 1)
            def _():
                spread(index, col_t.at[index], send_l, down).start()

    first = (z == 0) & (c == 0)
    order = (4, 1, 7, 2, 6, 3, 5, 0)

    def across(d):
        b = (y + d) % 8
        return remote(
            moved.at[b, pl.ds(2 * (1 - xl), 2)], half.at[b], sx.at[d], rx.at[d], grp=g ^ 1
        )

    def along(d):
        b = (y + d) % 8
        return remote(mine.at[b], parts.at[d], sy.at[d], ry.at[d], grp=(g + 2 * d) % 16)

    def combine(j):
        b = j // 4 * 4 + mapping[0, 8 * c + j] % 4
        moved[j] = dot(left[b], col_t[b]).reshape(4, BLK, BLK)

    last = PAIRS.index((4, 4))

    @pl.when(jnp.logical_not(first))
    def _():
        @pl.when((z == 1) & (c == 0))
        def _():
            combine(4)
            remote(moved.at[4, 0], lblk.at[last], se, re, row=0).start()

        for d in order:
            j = (y + d) % 8

            @pl.when(jnp.logical_not((z == 1) & (c == 0) & (j == 4)))
            def _():
                combine(j)

            across(d).start()

    @pl.when(first)
    def _():
        for j in range(NPAN):
            combine(j)
        for t, (i, j) in enumerate(PAIRS[:last]):
            lblk[t] = moved[j, i]
        for d in order:
            k = (y + d) % 8
            t = 2 * k + 1 - xl

            @pl.when(t == last)
            def _():
                arrived(lblk.at[last], se, re)

            @pl.when(t < NPAIR)
            def _():
                remote(lblk.at[t], lx.at[k], sl1.at[k], rl1.at[k], grp=g ^ 1).start()

        for d in order:
            k = (y + d) % 8
            t = 2 * k + xl

            @pl.when(t == last)
            def _():
                arrived(lblk.at[last], se, re)

            @pl.when(t < NPAIR)
            def _():
                arrived(lx.at[k], sl1.at[k], rl1.at[k])
                lsum[k] = lblk[t] + lx[k]
                if d:
                    remote(lsum.at[k], lparts.at[d], s1.at[d], r1.at[d], grp=(g + 2 * d) % 16).start()

        for j in range(NPAN, 8):
            combine(j)
        for d in order:
            across(d).start()

    def among_members():
        for d in GRP_FAR:
            remote(lead.at[g], lead.at[g], s3.at[d], r3.at[g], grp=(g + d) % 16).start()
        remote(lead.at[g], lead.at[g], s4.at[0], r4.at[g], col=c ^ 1).start()

    def to_rows(d):
        return (
            remote(total, lead.at[g], s2.at[d], r2, row=(z + d) % 8, col=2),
            remote(total, lead.at[g], s2.at[8 + d], r2, row=(z + d) % 8, col=0),
        )

    @pl.when(first & (g < NPAIR))
    def _():
        acc = lsum[y]
        for d in order[:-1]:
            arrived(lparts.at[d], s1.at[d], r1.at[d])
            acc = acc + lparts[d]
        total[...] = acc
        lead[g] = acc
        for d in FAR + (0,):
            for copy in to_rows(d)[: 2 if d else 1]:
                copy.start()

    late = first | ((c == 2) & (z < 3))
    for turn, d in enumerate(order):
        b = (y + d) % 8
        across(d).wait_recv()
        mine[b] = moved[b, pl.ds(2 * xl, 2)] + half[b]
        if d:
            along(d).start()
        if turn == 5:
            @pl.when((core == 0) & (g < NPAIR) & jnp.logical_not(late))
            def _():
                arrived(lead.at[g], s2.at[0], r2)
                among_members()

    @pl.when((core == 0) & (g < NPAIR) & late)
    def _():
        @pl.when(jnp.logical_not(first))
        def _():
            arrived(lead.at[g], s2.at[0], r2)

        among_members()

    acc = mine[y]
    for d in order[:-1]:
        along(d).wait_recv()
        acc = acc + parts[d]
    own[...] = acc

    for src_z, src_xl, start, count in COL_SOURCES:
        n = src_z * 2 + src_xl
        there = by_col.at[pl.ds(start, count)]
        src = own.at[pl.ds(0, count)]

        @pl.when((z == src_z) & (xl == src_xl))
        def _():
            for d in FAR:
                remote(src, there, sz.at[n, d], rz.at[n], row=(z + d) % 8).start()
            remote(src, there, sl.at[n], rl.at[n], grp=g ^ 1).start()
            by_col[start : start + count] = own[0:count]

    @pl.when((c == 0) & (y < NPAN))
    def _():
        remote(own, by_row.at[y], spx, rr.at[y], col=2).start()
        for d in FAR:
            remote(own, by_row.at[y], spy.at[d], rr.at[y], grp=(g + 2 * d) % 16).start()
        remote(own, by_row.at[y], sc.at[y], rcd.at[y], col=c ^ 1).start()
        by_row[y] = own[...]

    @pl.when(core == 0)
    def _():
        for d in GRP_FAR:
            t = (g + 16 - d) % 16

            @pl.when(t < NPAIR)
            def _():
                arrived(lead.at[t], s3.at[0], r3.at[t])
                remote(lead.at[t], lead.at[t], s4.at[16 - d], r4.at[t], col=c ^ 1).start()

    @pl.when(core == 1)
    def _():
        for t in range(NPAIR):
            arrived(lead.at[t], s4.at[0], r4.at[t])

    for t, (i, j) in enumerate(PAIRS):
        square[i * BLK : (i + 1) * BLK, j * BLK : (j + 1) * BLK] = lead[t]

    def factor(k):
        low, high = k * BLK, (k + 1) * BLK
        inverse[k] = factor_inverse(square[low:high, low:high])
        if k + 1 < NPAN:
            across_panel = dot(inverse[k], square[low:high, high:])
            upper[low:high, high:] = across_panel
            square[high:, high:] -= dot(across_panel.T, across_panel)

    factor(0)

    @pl.when((c == 2) & (y < NPAN))
    def _():
        arrived(by_row.at[y], spx, rr.at[y])
        for d in FAR:
            remote(by_row.at[y], by_row.at[y], spy.at[d], rr.at[y], grp=(g + 2 * d) % 16).start()
        remote(by_row.at[y], by_row.at[y], sc.at[y], rcd.at[y], col=c ^ 1).start()

    factor(1)
    factor(2)
    for src_z, src_xl, start, count in COL_SOURCES:
        n = src_z * 2 + src_xl
        there = by_col.at[pl.ds(start, count)]

        @pl.when((z != src_z) & (xl == src_xl))
        def _():
            arrived(there, sz.at[n, 0], rz.at[n])
            remote(there, there, sl.at[n], rl.at[n], grp=g ^ 1).start()

    factor(3)

    @pl.when(core == 0)
    def _():
        for k in range(NPAN):
            @pl.when(y != k)
            def _():
                arrived(by_row.at[k], spx, rr.at[k])
                remote(by_row.at[k], by_row.at[k], sc.at[k], rcd.at[k], col=c ^ 1).start()

    for src_z, src_xl, start, count in COL_SOURCES:
        n = src_z * 2 + src_xl

        @pl.when(xl != src_xl)
        def _():
            arrived(by_col.at[pl.ds(start, count)], sl.at[n], rl.at[n])

    @pl.when(core == 1)
    def _():
        for k in range(NPAN):
            arrived(by_row.at[k], sc.at[k], rcd.at[k])

    row_block = 4 * z + 2 * xl
    col_block = 8 * c + y
    which = row_block + lax.broadcasted_iota(jnp.int32, (2 * BLK, BLK), 0) // BLK
    for k in range(NPAN):
        rows[:, k * BLK : (k + 1) * BLK] = by_row[k].reshape(2 * BLK, BLK)
    cols[...] = by_col[...].reshape(NPAN * BLK, BLK)
    panel_piece = jnp.zeros((2 * BLK, BLK), jnp.float32)
    rest = own[...].reshape(2 * BLK, BLK)
    factor(4)
    for k in range(NPAN):
        low, high = k * BLK, (k + 1) * BLK
        col_factor = dot(inverse[k], cols[low:high])
        row_factor = jnp.where(which >= k, dot_nt(rows[:, low:high], inverse[k]), 0.0)
        panel_piece = jnp.where(col_block == k, row_factor, panel_piece)
        if k + 1 < NPAN:
            across_panel = upper[low:high, high:]
            cols[high:] -= dot(across_panel.T, col_factor)
            rows[:, high:] -= dot(row_factor, across_panel)
        rest = rest - dot(row_factor, col_factor)
    piece[...] = jnp.where(col_block < NPAN, panel_piece, rest).reshape(2, BLK, BLK)

    to = {"x": g ^ 1, "r": (g + 2) % 16, "l": (g + 14) % 16}

    def spot(x, steps, part):
        row = pl.multiple_of((x * 2 + part) * BLK, BLK)
        col = pl.multiple_of(((y - steps + 8) % 8) * BLK, BLK)
        return out.at[pl.ds(row, BLK), pl.ds(col, BLK)]

    def here(name, part):
        other, steps = HOPS[name]
        return spot(1 - xl if other else xl, steps, part)

    def hop(src_name, name, way, part):
        if src_name == "own":
            src, dst = piece.at[part], spot(xl, 0, part)
        else:
            src = dst = here(src_name, part)
        n = NAMES.index(name)
        return remote(src, dst, send6.at[n, part], recv6.at[n, part], grp=to[way])

    for part in range(2):
        for name, way in ONWARD["own"]:
            hop("own", name, way, part).start()
        row = pl.multiple_of((xl * 2 + part) * BLK, BLK)
        out[pl.ds(row, BLK), pl.ds(pl.multiple_of(y * BLK, BLK), BLK)] = piece[part]
    for src_name in list(ONWARD)[1:]:
        for part in range(2):
            n = NAMES.index(src_name)
            arrived(here(src_name, part), send6.at[n, part], recv6.at[n, part])
            for name, way in ONWARD[src_name]:
                hop(src_name, name, way, part).start()
    for src_name in ONWARD:
        for name, way in ONWARD[src_name]:
            for part in range(2):
                hop(src_name, name, way, part).wait_send()

    for slot in range(2):
        away = away_of(slot)
        for part in range(4):
            index = slot * 4 + part

            @pl.when(away < reach)
            def _():
                spread(index, col_t.at[index], send_r, up).wait_send()

            @pl.when((away > reach + 1) | (away == 0))
            def _():
                spread(index, col_t.at[index], send_l, down).wait_send()
    for d in order:
        across(d).wait_send()
        if d:
            along(d).wait_send()

    @pl.when((z == 1) & (c == 0))
    def _():
        remote(total, total, se, re, row=0).wait_send()

    @pl.when(first)
    def _():
        for d in order:
            k = (y + d) % 8

            @pl.when(2 * k + 1 - xl < NPAIR)
            def _():
                remote(total, total, sl1.at[k], rl1.at[k], grp=g ^ 1).wait_send()

            if d:
                @pl.when(2 * k + xl < NPAIR)
                def _():
                    remote(total, total, s1.at[d], r1.at[d], grp=g ^ 1).wait_send()

        @pl.when(g < NPAIR)
        def _():
            for d in FAR + (0,):
                for copy in to_rows(d)[: 2 if d else 1]:
                    copy.wait_send()

    for src_z, src_xl, start, count in COL_SOURCES:
        n = src_z * 2 + src_xl
        there = by_col.at[pl.ds(start, count)]

        @pl.when(xl == src_xl)
        def _():
            @pl.when(z == src_z)
            def _():
                for d in FAR:
                    remote(there, there, sz.at[n, d], rz.at[n], row=(z + d) % 8).wait_send()
            remote(there, there, sl.at[n], rl.at[n], grp=g ^ 1).wait_send()

    @pl.when(core == 0)
    def _():
        @pl.when(y < NPAN)
        def _():
            @pl.when(c == 0)
            def _():
                remote(own, by_row.at[y], spx, rr.at[y], col=2).wait_send()
            for d in FAR:
                remote(own, by_row.at[y], spy.at[d], rr.at[y], grp=(g + 2 * d) % 16).wait_send()
        for k in range(NPAN):
            remote(own, by_row.at[k], sc.at[k], rcd.at[k], col=c ^ 1).wait_send()

        @pl.when(g < NPAIR)
        def _():
            for d in GRP_FAR:
                remote(total, lead.at[g], s3.at[d], r3.at[g], grp=(g + d) % 16).wait_send()
        for d in range(16):
            t = (g + d) % 16

            @pl.when(t < NPAIR)
            def _():
                remote(total, lead.at[t], s4.at[d], r4.at[t], col=c ^ 1).wait_send()


def whole(mapping, own_t, normal):
    dma = pltpu.SemaphoreType.DMA

    def buf(*shape):
        return pltpu.VMEM(shape, jnp.float32)

    order = NPAN * BLK
    hbm = pl.BlockSpec(memory_space=pltpu.HBM)
    return pl.pallas_call(
        whole_kernel,
        out_shape=f32(4 * BLK, 8 * BLK),
        in_specs=[pl.BlockSpec(memory_space=pltpu.SMEM), hbm, hbm],
        out_specs=VMEM,
        scratch_shapes=[
            buf(NPAIR, BLK, BLK), buf(2, BLK, BLK), buf(NPAN, 2, BLK, BLK), buf(NPAN, BLK, BLK),
            buf(4, BLK, BLK), buf(4, BLK, 8 * BLK), buf(8, BLK, BLK), buf(8, 4 * BLK, BLK), buf(8, 4, BLK, BLK),
            buf(8, 2, BLK, BLK), buf(8, 2, BLK, BLK), buf(8, 2, BLK, BLK),
            buf(8, BLK, BLK), buf(NPAIR, BLK, BLK), buf(8, BLK, BLK), buf(8, BLK, BLK), buf(BLK, BLK),
            buf(order, order), buf(order, order), buf(NPAN, BLK, BLK), buf(2 * BLK, order), buf(order, BLK),
            buf(2, BLK, BLK),
            dma, dma, dma((8,)), dma((8,)), dma((8,)), dma((8,)), dma((8,)), dma((8,)), dma((8,)),
            dma((16,)), dma((16,)), dma, dma, dma((16,)), dma, dma((16,)), dma((16,)), dma((16,)), dma((16,)),
            dma, dma((NPAN,)), dma((8,)), dma((NPAN,)), dma((NPAN,)), dma((3, 8)), dma((3,)), dma((3,)), dma((3,)),
            dma((15, 2)), dma((15, 2)), dma((8,)), dma((8,)),
        ],
        compiler_params=params(1),
    )(mapping, own_t, normal)


def on_device(normals, transforms, block_map):
    return whole(block_map, transforms[0], normals.reshape(4, BLK, 8 * BLK))


def solution(mesh):
    return jax.shard_map(
        on_device,
        mesh=mesh,
        in_specs=(P("grp", "row", "col"), P("grp", "row", None, None), P("grp", None)),
        out_specs=P("row", "col"),
        check_vma=False,
    )
```

```python
import functools

import jax
import jax.numpy as jnp
from jax import lax
from jax.experimental import pallas as pl
from jax.experimental.pallas import tpu as pltpu
from jax.sharding import PartitionSpec as P

BLK = 128
NPAN = 5
STEP = 8
HALF = 64
MESH = pl.DeviceIdType.MESH
HIGHEST = lax.Precision.HIGHEST
VMEM = pl.BlockSpec(memory_space=pltpu.VMEM)
PAIRS = [(i, j) for i in range(NPAN) for j in range(i, NPAN)]
NPAIR = len(PAIRS)


def f32(*shape):
    return jax.ShapeDtypeStruct(shape, jnp.float32)


def place():
    grp = lax.axis_index("grp")
    col = lax.axis_index("col")
    return dict(
        g=grp, y=grp // 2, xl=grp % 2, z=lax.axis_index("row"), c=col, xh=col // 2, core=col % 2
    )


def remote(src, dst, send, recv, **where):
    return pltpu.make_async_remote_copy(
        src_ref=src, dst_ref=dst, send_sem=send, recv_sem=recv, device_id=where, device_id_type=MESH
    )


def arrived(dst, send, recv):
    remote(dst, dst, send, recv, grp=lax.axis_index("grp")).wait_recv()


def meet(partners):
    barrier = pltpu.get_barrier_semaphore()
    for where in partners:
        pl.semaphore_signal(barrier, inc=1, device_id=where, device_id_type=MESH)
    pl.semaphore_wait(barrier, len(partners))


def params(ident):
    return pltpu.CompilerParams(collective_id=ident, has_side_effects=True, vmem_limit_bytes=53300000)


FAR = (4, 3, 5, 2, 6, 1, 7)
GRP_FAR = (8, 7, 9, 6, 10, 5, 11, 4, 12, 3, 13, 2, 14, 1, 15)
COL_SOURCES = ((0, 0, 0, 2), (0, 1, 2, 2), (1, 0, 4, 1))


def dot(a, b):
    return jnp.dot(a, b, precision=HIGHEST, preferred_element_type=jnp.float32)


def factor_inverse(a):
    row_ids = lax.broadcasted_iota(jnp.int32, (BLK, BLK), 0)
    col_ids = lax.broadcasted_iota(jnp.int32, (BLK, BLK), 1)
    done = []
    for start in range(0, BLK, STEP):
        rest = BLK - start
        cols = [jnp.broadcast_to(a[:, start + j : start + j + 1], (rest, BLK)) for j in range(STEP)]
        here = (col_ids[start:] >= start) & (col_ids[start:] < start + STEP)
        unit = jnp.where(col_ids[start:] == row_ids[start:], 1.0, 0.0).astype(jnp.float32)
        a = jnp.where(here, unit, a)
        top = a[:STEP]
        rows = []
        for j in range(STEP):
            scale = lax.rsqrt(cols[j][j : j + 1])
            cols[j] = cols[j] * scale
            row = top[j : j + 1] * scale
            rows.append(row)
            if j + 1 < STEP:
                top = top - cols[j][:STEP] * row
                for k in range(j + 1, STEP):
                    cols[k] = cols[k] - cols[j][k : k + 1] * cols[j]
        done.append(jnp.concatenate(rows, axis=0))
        if rest > STEP:
            a = a[STEP:]
            for j in range(STEP):
                a = a - cols[j][STEP:] * rows[j]
    return jnp.where(col_ids <= row_ids, jnp.concatenate(done, axis=0), 0.0)


def dot_nt(a, b):
    return lax.dot_general(
        a, b, (((1,), (1,)), ((), ())), precision=HIGHEST, preferred_element_type=jnp.float32
    )


HOPS = {
    "R1": (0, 1), "R2": (0, 2), "R3": (0, 3), "R4": (0, 4), "L1": (0, -1), "L2": (0, -2), "L3": (0, -3),
    "P0": (1, 0), "RP1": (1, 1), "LP1": (1, -1), "LP2": (1, -2),
    "X2": (1, 2), "X3": (1, 3), "X4": (1, 4), "XL": (1, -3),
}
NAMES = list(HOPS)
ONWARD = {
    "own": (("P0", "x"), ("R1", "r"), ("L1", "l")),
    "P0": (("RP1", "r"), ("LP1", "l")),
    "R1": (("R2", "r"),),
    "L1": (("L2", "l"),),
    "R2": (("R3", "r"), ("X2", "x")),
    "L2": (("L3", "l"),),
    "LP1": (("LP2", "l"),),
    "R3": (("R4", "r"), ("X3", "x")),
    "L3": (("XL", "x"),),
    "R4": (("X4", "x"),),
    "RP1": (), "LP2": (), "X2": (), "XL": (), "X3": (), "X4": (),
}


def whole_kernel(
    mapping, own_t_hbm, normal_hbm, out,
    lead, own, by_row, by_col, own_t, normal, col_t, left, moved, half, mine, parts, lparts, lblk, lx, lsum, total,
    square, upper, inverse, rows, cols, piece, sem_t,
    sem, send_r, send_l, recv, sx, rx, sy, ry,
    s1, r1, se, re, s2, r2, s3, r3, s4, r4, spx, rr, spy, sc, rcd, sz, rz, sl, rl,
    send6, recv6, sl1, rl1, s5,
):
    me = place()
    g, y, xl, z, c, core = me["g"], me["y"], me["xl"], me["z"], me["c"], me["core"]
    fetch_t = pltpu.make_async_copy(own_t_hbm, own_t, sem_t)
    fetch_t.start()
    fetch = pltpu.make_async_copy(normal_hbm, normal, sem)
    fetch.start()
    meet(
        [{"grp": (g + d) % 16} for d in range(1, 16)]
        + [{"row": (z + d) % 8} for d in range(1, 8)]
        + [{"col": c ^ 1}]
        + [{"row": (z + d) % 8, "col": c ^ 2} for d in range(8)]
    )

    fetch_t.wait()

    up, down = (z + 1) % 8, (z + 7) % 8
    reach = 4 - core

    def away_of(slot):
        return (z - (2 * c + slot) + 8) % 8

    def spread(index, src, sends, to):
        return remote(src, col_t.at[index], sends.at[index], recv.at[index], row=to)

    for slot in range(2):
        @pl.when(away_of(slot) == 0)
        def _():
            for part in range(4):
                index = slot * 4 + part
                spread(index, own_t.at[part], send_r, up).start()
                spread(index, own_t.at[part], send_l, down).start()
                col_t[index] = own_t[part]

    fetch.wait()
    for i in range(4):
        block = mapping[0, 4 * z + i] % 4
        turned = dot(own_t[block].T, normal[block])
        for b in range(8):
            left[b, i * BLK : (i + 1) * BLK, :] = turned[:, b * BLK : (b + 1) * BLK]

    rising = (away_of(1) <= reach).astype(jnp.int32)
    for part in range(4):
        for turn in range(2):
            slot = (rising + turn) % 2
            index = slot * 4 + part
            away = away_of(slot)

            @pl.when(away != 0)
            def _():
                arrived(col_t.at[index], send_r.at[index], recv.at[index])

            @pl.when((away > 0) & (away < reach))
            def _():
                spread(index, col_t.at[index], send_r, up).start()

            @pl.when(away > reach + 1)
            def _():
                spread(index, col_t.at[index], send_l, down).start()

    first = (z == 0) & (c == 0)
    order = (4, 1, 7, 2, 6, 3, 5, 0)

    def across(d):
        b = (y + d) % 8
        return remote(
            moved.at[b, pl.ds(2 * (1 - xl), 2)], half.at[b], sx.at[d], rx.at[d], grp=g ^ 1
        )

    def along(d):
        b = (y + d) % 8
        return remote(mine.at[b], parts.at[d], sy.at[d], ry.at[d], grp=(g + 2 * d) % 16)

    def combine(j):
        b = j // 4 * 4 + mapping[0, 8 * c + j] % 4
        moved[j] = dot(left[b], col_t[b]).reshape(4, BLK, BLK)

    last = PAIRS.index((4, 4))

    @pl.when(jnp.logical_not(first))
    def _():
        @pl.when((z == 1) & (c == 0))
        def _():
            combine(4)
            remote(moved.at[4, 0], lblk.at[last], se, re, row=0).start()

        for d in order:
            j = (y + d) % 8

            @pl.when(jnp.logical_not((z == 1) & (c == 0) & (j == 4)))
            def _():
                combine(j)

            across(d).start()

    @pl.when(first)
    def _():
        for j in range(NPAN):
            combine(j)
        for t, (i, j) in enumerate(PAIRS[:last]):
            lblk[t] = moved[j, i]
        for d in order:
            k = (y + d) % 8
            t = 2 * k + 1 - xl

            @pl.when(t == last)
            def _():
                arrived(lblk.at[last], se, re)

            @pl.when(t < NPAIR)
            def _():
                remote(lblk.at[t], lx.at[k], sl1.at[k], rl1.at[k], grp=g ^ 1).start()

        for d in order:
            k = (y + d) % 8
            t = 2 * k + xl

            @pl.when(t == last)
            def _():
                arrived(lblk.at[last], se, re)

            @pl.when(t < NPAIR)
            def _():
                arrived(lx.at[k], sl1.at[k], rl1.at[k])
                lsum[k] = lblk[t] + lx[k]
                if d:
                    remote(lsum.at[k], lparts.at[d], s1.at[d], r1.at[d], grp=(g + 2 * d) % 16).start()

        for j in range(NPAN, 8):
            combine(j)
        for d in order:
            across(d).start()

    def to_members():
        for d in GRP_FAR:
            copy = remote(lead.at[g], lead.at[g], s3.at[d], r3.at[g], grp=(g + d) % 16)
            yield (((g + d) % 16) // 2 - y + 8) % 8 != 4, copy

    def among_members():
        for near, copy in to_members():
            @pl.when(near)
            def _():
                copy.start()

        remote(lead.at[g], lead.at[g], s4.at[0], r4.at[g], col=c ^ 1).start()

    def to_rows(d):
        return (
            remote(total, lead.at[g], s2.at[d], r2, row=(z + d) % 8, col=2),
            remote(total, lead.at[g], s2.at[8 + d], r2, row=(z + d) % 8, col=0),
        )

    @pl.when(first & (g < NPAIR))
    def _():
        acc = lsum[y]
        for d in order[:-1]:
            arrived(lparts.at[d], s1.at[d], r1.at[d])
            acc = acc + lparts[d]
        total[...] = acc
        lead[g] = acc
        for d in FAR + (0,):
            for copy in to_rows(d)[: 2 if d else 1]:
                copy.start()

    late = (c == 2) & (z < 3)
    for turn, d in enumerate(order):
        b = (y + d) % 8
        across(d).wait_recv()
        mine[b] = moved[b, pl.ds(2 * xl, 2)] + half[b]
        if d:
            along(d).start()
        if turn == 5:
            @pl.when((core == 0) & (g < NPAIR) & jnp.logical_not(late))
            def _():
                @pl.when(jnp.logical_not(first))
                def _():
                    arrived(lead.at[g], s2.at[0], r2)

                among_members()

    @pl.when((core == 0) & (g < NPAIR) & late)
    def _():
        arrived(lead.at[g], s2.at[0], r2)
        among_members()

    acc = mine[y]
    for d in order[:-1]:
        along(d).wait_recv()
        acc = acc + parts[d]
    own[...] = acc

    for src_z, src_xl, start, count in COL_SOURCES:
        n = src_z * 2 + src_xl
        there = by_col.at[pl.ds(start, count)]
        src = own.at[pl.ds(0, count)]

        @pl.when((z == src_z) & (xl == src_xl))
        def _():
            for d in FAR:
                remote(src, there, sz.at[n, d], rz.at[n], row=(z + d) % 8).start()
            remote(src, there, sl.at[n], rl.at[n], grp=g ^ 1).start()
            by_col[start : start + count] = own[0:count]

    @pl.when((c == 0) & (y < NPAN))
    def _():
        remote(own, by_row.at[y], spx, rr.at[y], col=2).start()
        for d in FAR:
            remote(own, by_row.at[y], spy.at[d], rr.at[y], grp=(g + 2 * d) % 16).start()
        remote(own, by_row.at[y], sc.at[y], rcd.at[y], col=c ^ 1).start()
        by_row[y] = own[...]

    def passed(t, q):
        return remote(lead.at[t], lead.at[t], s5.at[q], r3.at[t], grp=(g + 14) % 16)

    @pl.when(core == 0)
    def _():
        for q in range(2):
            t = (y + 3) % 8 * 2 + q

            @pl.when(t < NPAIR)
            def _():
                arrived(lead.at[t], s3.at[0], r3.at[t])
                passed(t, q).start()
                remote(lead.at[t], lead.at[t], s4.at[(t - g + 16) % 16], r4.at[t], col=c ^ 1).start()

        for d in GRP_FAR:
            t = (g + 16 - d) % 16

            @pl.when((t < NPAIR) & (t // 2 != (y + 3) % 8))
            def _():
                arrived(lead.at[t], s3.at[0], r3.at[t])
                remote(lead.at[t], lead.at[t], s4.at[16 - d], r4.at[t], col=c ^ 1).start()

    @pl.when(core == 1)
    def _():
        for t in range(NPAIR):
            arrived(lead.at[t], s4.at[0], r4.at[t])

    for t, (i, j) in enumerate(PAIRS):
        square[i * BLK : (i + 1) * BLK, j * BLK : (j + 1) * BLK] = lead[t]

    def factor(k):
        low, high = k * BLK, (k + 1) * BLK
        inverse[k] = factor_inverse(square[low:high, low:high])
        if k + 1 < NPAN:
            across_panel = dot(inverse[k], square[low:high, high:])
            upper[low:high, high:] = across_panel
            square[high:, high:] -= dot(across_panel.T, across_panel)

    factor(0)

    @pl.when((c == 2) & (y < NPAN))
    def _():
        arrived(by_row.at[y], spx, rr.at[y])
        for d in FAR:
            remote(by_row.at[y], by_row.at[y], spy.at[d], rr.at[y], grp=(g + 2 * d) % 16).start()
        remote(by_row.at[y], by_row.at[y], sc.at[y], rcd.at[y], col=c ^ 1).start()

    factor(1)
    factor(2)
    for src_z, src_xl, start, count in COL_SOURCES:
        n = src_z * 2 + src_xl
        there = by_col.at[pl.ds(start, count)]

        @pl.when((z != src_z) & (xl == src_xl))
        def _():
            arrived(there, sz.at[n, 0], rz.at[n])
            remote(there, there, sl.at[n], rl.at[n], grp=g ^ 1).start()

    factor(3)

    @pl.when(core == 0)
    def _():
        for k in range(NPAN):
            @pl.when(y != k)
            def _():
                arrived(by_row.at[k], spx, rr.at[k])
                remote(by_row.at[k], by_row.at[k], sc.at[k], rcd.at[k], col=c ^ 1).start()

    for src_z, src_xl, start, count in COL_SOURCES:
        n = src_z * 2 + src_xl

        @pl.when(xl != src_xl)
        def _():
            arrived(by_col.at[pl.ds(start, count)], sl.at[n], rl.at[n])

    @pl.when(core == 1)
    def _():
        for k in range(NPAN):
            arrived(by_row.at[k], sc.at[k], rcd.at[k])

    row_block = 4 * z + 2 * xl
    col_block = 8 * c + y
    which = row_block + lax.broadcasted_iota(jnp.int32, (2 * BLK, BLK), 0) // BLK
    for k in range(NPAN):
        rows[:, k * BLK : (k + 1) * BLK] = by_row[k].reshape(2 * BLK, BLK)
    cols[...] = by_col[...].reshape(NPAN * BLK, BLK)
    panel_piece = jnp.zeros((2 * BLK, BLK), jnp.float32)
    rest = own[...].reshape(2 * BLK, BLK)
    factor(4)
    for k in range(NPAN):
        low, high = k * BLK, (k + 1) * BLK
        col_factor = dot(inverse[k], cols[low:high])
        row_factor = jnp.where(which >= k, dot_nt(rows[:, low:high], inverse[k]), 0.0)
        panel_piece = jnp.where(col_block == k, row_factor, panel_piece)
        if k + 1 < NPAN:
            across_panel = upper[low:high, high:]
            cols[high:] -= dot(across_panel.T, col_factor)
            rows[:, high:] -= dot(row_factor, across_panel)
        rest = rest - dot(row_factor, col_factor)
    piece[...] = jnp.where(col_block < NPAN, panel_piece, rest).reshape(4, HALF, BLK)

    to = {"x": g ^ 1, "r": (g + 2) % 16, "l": (g + 14) % 16}

    def spot(x, steps, part):
        row = pl.multiple_of((x * 4 + part) * HALF, HALF)
        col = pl.multiple_of(((y - steps + 8) % 8) * BLK, BLK)
        return out.at[pl.ds(row, HALF), pl.ds(col, BLK)]

    def here(name, part):
        other, steps = HOPS[name]
        return spot(1 - xl if other else xl, steps, part)

    def hop(src_name, name, way, part):
        if src_name == "own":
            src, dst = piece.at[part], spot(xl, 0, part)
        else:
            src = dst = here(src_name, part)
        n = NAMES.index(name)
        return remote(src, dst, send6.at[n, part], recv6.at[n, part], grp=to[way])

    for part in range(4):
        for name, way in ONWARD["own"]:
            hop("own", name, way, part).start()
        row = pl.multiple_of((xl * 4 + part) * HALF, HALF)
        out[pl.ds(row, HALF), pl.ds(pl.multiple_of(y * BLK, BLK), BLK)] = piece[part]
    for src_name in list(ONWARD)[1:]:
        for part in range(4):
            n = NAMES.index(src_name)
            arrived(here(src_name, part), send6.at[n, part], recv6.at[n, part])
            for name, way in ONWARD[src_name]:
                hop(src_name, name, way, part).start()
    for src_name in ONWARD:
        for name, way in ONWARD[src_name]:
            for part in range(4):
                hop(src_name, name, way, part).wait_send()

    for slot in range(2):
        away = away_of(slot)
        for part in range(4):
            index = slot * 4 + part

            @pl.when(away < reach)
            def _():
                spread(index, col_t.at[index], send_r, up).wait_send()

            @pl.when((away > reach + 1) | (away == 0))
            def _():
                spread(index, col_t.at[index], send_l, down).wait_send()
    for d in order:
        across(d).wait_send()
        if d:
            along(d).wait_send()

    @pl.when((z == 1) & (c == 0))
    def _():
        remote(total, total, se, re, row=0).wait_send()

    @pl.when(first)
    def _():
        for d in order:
            k = (y + d) % 8

            @pl.when(2 * k + 1 - xl < NPAIR)
            def _():
                remote(total, total, sl1.at[k], rl1.at[k], grp=g ^ 1).wait_send()

            if d:
                @pl.when(2 * k + xl < NPAIR)
                def _():
                    remote(total, total, s1.at[d], r1.at[d], grp=g ^ 1).wait_send()

        @pl.when(g < NPAIR)
        def _():
            for d in FAR + (0,):
                for copy in to_rows(d)[: 2 if d else 1]:
                    copy.wait_send()

    for src_z, src_xl, start, count in COL_SOURCES:
        n = src_z * 2 + src_xl
        there = by_col.at[pl.ds(start, count)]

        @pl.when(xl == src_xl)
        def _():
            @pl.when(z == src_z)
            def _():
                for d in FAR:
                    remote(there, there, sz.at[n, d], rz.at[n], row=(z + d) % 8).wait_send()
            remote(there, there, sl.at[n], rl.at[n], grp=g ^ 1).wait_send()

    @pl.when(core == 0)
    def _():
        @pl.when(y < NPAN)
        def _():
            @pl.when(c == 0)
            def _():
                remote(own, by_row.at[y], spx, rr.at[y], col=2).wait_send()
            for d in FAR:
                remote(own, by_row.at[y], spy.at[d], rr.at[y], grp=(g + 2 * d) % 16).wait_send()
        for k in range(NPAN):
            remote(own, by_row.at[k], sc.at[k], rcd.at[k], col=c ^ 1).wait_send()

        @pl.when(g < NPAIR)
        def _():
            for near, copy in to_members():
                @pl.when(near)
                def _():
                    copy.wait_send()

        for q in range(2):
            t = (y + 3) % 8 * 2 + q

            @pl.when(t < NPAIR)
            def _():
                passed(t, q).wait_send()

        for d in range(16):
            t = (g + d) % 16

            @pl.when(t < NPAIR)
            def _():
                remote(total, lead.at[t], s4.at[d], r4.at[t], col=c ^ 1).wait_send()


def whole(mapping, own_t, normal):
    dma = pltpu.SemaphoreType.DMA

    def buf(*shape):
        return pltpu.VMEM(shape, jnp.float32)

    order = NPAN * BLK
    hbm = pl.BlockSpec(memory_space=pltpu.HBM)
    return pl.pallas_call(
        whole_kernel,
        out_shape=f32(4 * BLK, 8 * BLK),
        in_specs=[pl.BlockSpec(memory_space=pltpu.SMEM), hbm, hbm],
        out_specs=VMEM,
        scratch_shapes=[
            buf(NPAIR, BLK, BLK), buf(2, BLK, BLK), buf(NPAN, 2, BLK, BLK), buf(NPAN, BLK, BLK),
            buf(4, BLK, BLK), buf(4, BLK, 8 * BLK), buf(8, BLK, BLK), buf(8, 4 * BLK, BLK), buf(8, 4, BLK, BLK),
            buf(8, 2, BLK, BLK), buf(8, 2, BLK, BLK), buf(8, 2, BLK, BLK),
            buf(8, BLK, BLK), buf(NPAIR, BLK, BLK), buf(8, BLK, BLK), buf(8, BLK, BLK), buf(BLK, BLK),
            buf(order, order), buf(order, order), buf(NPAN, BLK, BLK), buf(2 * BLK, order), buf(order, BLK),
            buf(4, HALF, BLK),
            dma, dma, dma((8,)), dma((8,)), dma((8,)), dma((8,)), dma((8,)), dma((8,)), dma((8,)),
            dma((16,)), dma((16,)), dma, dma, dma((16,)), dma, dma((16,)), dma((16,)), dma((16,)), dma((16,)),
            dma, dma((NPAN,)), dma((8,)), dma((NPAN,)), dma((NPAN,)), dma((3, 8)), dma((3,)), dma((3,)), dma((3,)),
            dma((15, 4)), dma((15, 4)), dma((8,)), dma((8,)), dma((2,)),
        ],
        compiler_params=params(1),
    )(mapping, own_t, normal)


def on_device(normals, transforms, block_map):
    return whole(block_map, transforms[0], normals.reshape(4, BLK, 8 * BLK))


def solution(mesh):
    return jax.shard_map(
        on_device,
        mesh=mesh,
        in_specs=(P("grp", "row", "col"), P("grp", "row", None, None), P("grp", None)),
        out_specs=P("row", "col"),
        check_vma=False,
    )
```
